512 devices in a mesh: ctx: 256 (over z, y, x_hi, core), tp: 2 (over x_lo).
Axes of the slice: x: 4 (x_hi: 2, x_lo: 2; x = x_hi * 2 + x_lo), y: 8, z: 8, core: 2. Of those that a mesh axis runs over, the one named last changes fastest.
Arguments:
- queries: bfloat16 [16384, 16, 128], P('ctx', 'tp'), may hold values from -6 to 6
- incoming_lookup_vectors: bfloat16 [16384, 4, 128], P('ctx', 'tp'), may hold values from -6 to 6
- incoming_content_vectors: bfloat16 [16384, 4, 128], P('ctx', 'tp'), may hold values from -6 to 6
Outputs:
- attention: bfloat16 [16384, 16, 128], P(('ctx', 'tp'))
- key_cache: bfloat16 [16384, 4, 128], P('ctx', 'tp')
The draws below stay inside these ranges and needn't reach their ends.
All inputs are finite; a program needn't handle non-finite values.
Results may differ from the reference program's by a relative error of at most 0.0075.
Values may be sent and summed in bfloat16 or wider, within the bound.
A program may use at most 128 MiB of HBM per device.

```python
import math
import jax
import jax.numpy as jnp
from jax import lax

ASKING_HEAD_COUNT = 16
SHARED_HEAD_COUNT = 4
HEAD_WIDTH = 128
SEQUENCE_LENGTH = 16384


def levels(stream_key, extent, shards, low, top_value):
    factor_of, own = 1.0, jax.random.fold_in(stream_key, 6)
    for axis_at, shards_of in shards:
        steps = jnp.exp(jax.random.uniform(jax.random.fold_in(own, axis_at), (shards_of,), jnp.float32, low / len(shards), top_value / len(shards)))
        factor_of = factor_of * jnp.repeat(steps, extent[axis_at] // shards_of).reshape([-1 if axis == axis_at else 1 for axis in range(len(extent))])
    return factor_of


def normal_values(own_key, dims, scale, bound, cuts=(), kind=jnp.bfloat16):
    entries = jax.random.normal(own_key, dims, jnp.float32) * scale
    if len(cuts) > 0:
        entries = levels(own_key, dims, cuts, -0.22, 0.18) * entries
    return jnp.clip(entries, min=-bound, max=bound).astype(kind)


def setup_inputs(seed: int = 0) -> dict:
    streams_of = jax.random.split(jax.random.key(seed), 4)
    queries = normal_values(streams_of[0], (SEQUENCE_LENGTH, ASKING_HEAD_COUNT, HEAD_WIDTH), 1.0, 6.0, ((0, 256), (1, 2)))
    incoming_lookup_vectors = normal_values(streams_of[1], (SEQUENCE_LENGTH, SHARED_HEAD_COUNT, HEAD_WIDTH), 1.0, 6.0, ((0, 256), (1, 2)))
    incoming_content_vectors = normal_values(streams_of[2], (SEQUENCE_LENGTH, SHARED_HEAD_COUNT, HEAD_WIDTH), 1.0, 6.0, ((0, 256), (1, 2)))
    return dict(queries=queries, incoming_lookup_vectors=incoming_lookup_vectors, incoming_content_vectors=incoming_content_vectors)


rope_base = 500000.0

def rotate(tensor, positions):
    feature_width = tensor.shape[-1]
    half_width = feature_width // 2
    inverse_freq = rope_base ** (-(jnp.arange(half_width, dtype=jnp.float32) * 2.0 / feature_width))
    angles = positions.astype(jnp.float32)[:, None] * inverse_freq[None, :]
    cosine = jnp.cos(angles)[:, None, :]
    sine_part = jnp.sin(angles)[:, None, :]
    widened = tensor.astype(jnp.float32)
    front_half = widened[..., :half_width]
    second = widened[..., half_width:]
    return jnp.concatenate([front_half * cosine - second * sine_part, second * cosine + front_half * sine_part], axis=-1).astype(jnp.bfloat16)

def reference(queries, incoming_lookup_vectors, incoming_content_vectors):
    seq_len = queries.shape[0]
    positions = jnp.arange(seq_len, dtype=jnp.int32)
    key_cache = rotate(incoming_lookup_vectors, positions)
    spun_vectors = rotate(queries, positions)
    heads_per_share = ASKING_HEAD_COUNT // SHARED_HEAD_COUNT
    score_scale = 1.0 / math.sqrt(HEAD_WIDTH)
    piece_height = math.gcd(seq_len, 1024)
    number_of_pieces = seq_len // piece_height
    gathered_heads = spun_vectors.reshape(number_of_pieces, piece_height, SHARED_HEAD_COUNT, heads_per_share, HEAD_WIDTH).transpose(2, 0, 1, 3, 4)
    block_starts = jnp.arange(number_of_pieces, dtype=jnp.int32) * piece_height

    def attend_group(operands):
        q_group, key_head, value_head = operands
        key_wide = key_head.astype(jnp.float32)
        value_wide = value_head.astype(jnp.float32)

        def attend_block(block_operands):
            q_block, block_start = block_operands
            row_pos = block_start + jnp.arange(piece_height, dtype=jnp.int32)
            causal = row_pos[:, None] >= positions[None, :]
            scores = jnp.einsum('sgd,td->gst', q_block.astype(jnp.float32), key_wide) * score_scale
            scores = jnp.where(causal[None], scores, -jnp.inf)
            weights = jax.nn.softmax(scores, axis=-1)
            return jnp.einsum('gst,td->sgd', weights, value_wide)
        return lax.map(attend_block, (q_group, block_starts))
    result = lax.map(attend_group, (gathered_heads, key_cache.transpose(1, 0, 2), incoming_content_vectors.transpose(1, 0, 2)))
    attention = result.transpose(1, 2, 0, 3, 4).reshape(seq_len, ASKING_HEAD_COUNT, HEAD_WIDTH).astype(jnp.bfloat16)
    return (attention, key_cache)
```

```python
import functools
import math

import jax
import jax.numpy as jnp
from jax import lax
from jax.experimental import pallas as pl
from jax.experimental.pallas import tpu as pltpu
from jax.sharding import PartitionSpec as P

MESH = pl.DeviceIdType.MESH
rope_base = 500000.0
RING = 8
CELLS = RING * RING
HALF = 64
PIECE = 2 * HALF
WIDTH = 128
GROUP = 4
ROWS = GROUP * PIECE
LAG = 2


def rotate(tensor, positions):
    feature_width = tensor.shape[-1]
    half_width = feature_width // 2
    inverse_freq = rope_base ** (-(jnp.arange(half_width, dtype=jnp.float32) * 2.0 / feature_width))
    angles = positions.astype(jnp.float32)[:, None] * inverse_freq[None, :]
    cosine = jnp.cos(angles)[:, None, :]
    sine_part = jnp.sin(angles)[:, None, :]
    widened = tensor.astype(jnp.float32)
    front_half = widened[..., :half_width]
    second = widened[..., half_width:]
    return jnp.concatenate(
        [front_half * cosine - second * sine_part, second * cosine + front_half * sine_part],
        axis=-1,
    ).astype(jnp.bfloat16)


def offset_of(k):
    return ((k + 1) // 2) * (1 - 2 * (k % 2))


def event_order():
    entries = [(i, 0, i) for i in range(1, 5)]
    for j in range(1, 4):
        for k in range(8):
            entries.append((j + abs(offset_of(k)), j, k))
    for k in range(4):
        entries.append((4 + abs(offset_of(2 * k + 1)), 4, k))
    entries.sort()
    return [(j, k) for _, j, k in entries]


ORDER = event_order()
EVENTS = len(ORDER)
PER_WORD = 5
WORDS = []
for first in range(0, EVENTS, PER_WORD):
    word = 0
    for place, (j, k) in enumerate(ORDER[first : first + PER_WORD]):
        word |= (j * 8 + k) << (6 * place)
    WORDS.append(word)


def decode(n):
    which = n // PER_WORD
    word = jnp.int32(WORDS[0])
    for at in range(1, len(WORDS)):
        word = jnp.where(which == at, jnp.int32(WORDS[at]), word)
    code = lax.shift_right_logical(word, 6 * (n - which * PER_WORD)) & 63
    j = code // 8
    k = code % 8
    first = j == 0
    last = j == 4
    odd = k % 2
    kl = jnp.where(first, 2 * k - 1, jnp.where(last, 2 * k + odd, k))
    kr = jnp.where(first, 2 * k, jnp.where(last, 2 * k + 1 - odd, k))
    return j, k, kl, kr


def kernel(q_ref, kv_ref, out_ref, buf, qbuf, obuf, acc, top, send_sem, own_sem, other_sem, swap_send, swap_recv, out_send, out_recv):
    ctx = lax.axis_index("ctx")
    tp = lax.axis_index("tp")
    core = ctx % 2
    xh = (ctx // 2) % 2
    cell = ctx // 4
    y = cell % RING
    z = cell // RING
    zfirst = core == 0
    my_a = jnp.where(zfirst, z, y)
    my_b = jnp.where(zfirst, y, z)
    stride_a = jnp.where(zfirst, RING, 1)
    stride_b = jnp.where(zfirst, 1, RING)

    def cell_at(a, b):
        return ((a + 2 * RING) % RING) * stride_a + ((b + 2 * RING) % RING) * stride_b

    def other_cell_at(a, b):
        return ((a + 2 * RING) % RING) * stride_b + ((b + 2 * RING) % RING) * stride_a

    def dev(at):
        return (at * 4 + xh * 2 + core, tp)

    a_up, a_down = dev(cell_at(my_a + 1, my_b)), dev(cell_at(my_a - 1, my_b))
    b_up, b_down = dev(cell_at(my_a, my_b + 1)), dev(cell_at(my_a, my_b - 1))
    mate = (cell * 4 + xh * 2 + 1 - core, tp)
    swap = (cell * 4 + (1 - xh) * 2 + core, tp)
    side = (ctx, 1 - tp)
    cross = (cell * 4 + (1 - xh) * 2 + core, 1 - tp)

    barrier = pltpu.get_barrier_semaphore()
    for device in (a_up, a_down, b_up, b_down, mate, swap, side, cross):
        pl.semaphore_signal(barrier, inc=1, device_id=device, device_id_type=MESH)
    pl.semaphore_wait(barrier, 8)

    mine = core * CELLS
    theirs = (1 - core) * CELLS
    own = mine + cell
    keep_rows = pl.ds(pl.multiple_of(xh * HALF, HALF), HALF)
    get_rows = pl.ds(pl.multiple_of((1 - xh) * HALF, HALF), HALF)

    def remote(src, dst, s_sem, r_sem, device):
        return pltpu.make_async_remote_copy(
            src_ref=src, dst_ref=dst, send_sem=s_sem, recv_sem=r_sem, device_id=device, device_id_type=MESH
        )

    kv_out = remote(kv_ref.at[1 - xh], buf.at[own, keep_rows], swap_send.at[0], swap_recv.at[0], swap)
    kv_out.start()
    ring_targets = (a_up, a_down, b_up, b_down)
    for device in ring_targets:
        remote(kv_ref.at[xh], buf.at[own, keep_rows], send_sem, own_sem.at[cell], device).start()
    remote(kv_ref.at[xh], buf.at[own, keep_rows], send_sem, other_sem.at[cell], mate).start()
    other_heads = pl.ds(pl.multiple_of((1 - xh) * GROUP, GROUP), GROUP)
    own_heads = pl.ds(pl.multiple_of(xh * GROUP, GROUP), GROUP)
    q_out = remote(q_ref.at[other_heads], qbuf.at[:, xh], swap_send.at[1], swap_recv.at[1], swap)
    q_out.start()
    buf[own, keep_rows] = kv_ref[xh]
    qbuf[:, xh] = q_ref[own_heads]

    remote(kv_ref.at[1 - xh], buf.at[own, get_rows], swap_send.at[0], swap_recv.at[0], swap).wait_recv()
    for device in ring_targets:
        remote(buf.at[own, get_rows], buf.at[own, get_rows], send_sem, own_sem.at[cell], device).start()
    remote(buf.at[own, get_rows], buf.at[own, get_rows], send_sem, other_sem.at[cell], mate).start()
    remote(q_ref.at[other_heads], qbuf.at[:, 1 - xh], swap_send.at[1], swap_recv.at[1], swap).wait_recv()

    factor = math.log2(math.e) / math.sqrt(WIDTH)

    def pass_on(at, device):
        spot = buf.at[mine + at]
        remote(spot, spot, send_sem, own_sem.at[at], device).start()

    def share(at):
        spot = buf.at[mine + at]
        remote(spot, spot, send_sem, other_sem.at[at], mate).start()

    def wait_own(at):
        spot = buf.at[mine + at]
        remote(spot, spot, send_sem, own_sem.at[at], b_up).wait_recv()

    def wait_other(at):
        spot = buf.at[theirs + at]
        remote(spot, spot, send_sem, other_sem.at[at], mate).wait_recv()

    def scores_of(keys):
        q = qbuf[...].reshape(ROWS, WIDTH)
        return lax.dot_general(q, keys, (((1,), (1,)), ((), ())), preferred_element_type=jnp.float32) * factor

    def row_max(parts):
        most = parts[0]
        for part in parts[1:]:
            most = jnp.maximum(most, part)
        return jnp.broadcast_to(jnp.max(most, axis=1, keepdims=True), (ROWS, WIDTH))

    wait_other(cell)
    row = lax.broadcasted_iota(jnp.int32, (ROWS, WIDTH), 0) % PIECE
    col = lax.broadcasted_iota(jnp.int32, (ROWS, WIDTH), 1)
    row_at = jnp.where(row < HALF, row, row + HALF) + core * HALF
    parts = []
    for piece, which in ((own, core), (theirs + cell, 1 - core)):
        col_at = jnp.where(col < HALF, col, col + HALF) + which * HALF
        s = scores_of(buf[piece, :, :WIDTH])
        parts.append(jnp.where(row_at >= col_at, s, -jnp.inf))
    most = row_max(parts)
    top[...] = most
    ones = jnp.ones((PIECE, WIDTH), jnp.bfloat16)
    total = None
    for part, piece in zip(parts, (own, theirs + cell)):
        p = jnp.exp2(part - most).astype(jnp.bfloat16)
        v = jnp.concatenate([buf[piece, :, WIDTH:], ones], axis=1)
        term = jnp.dot(p, v, preferred_element_type=jnp.float32)
        total = term if total is None else total + term
    acc[...] = total

    def attend(pieces):
        some = pieces[0][1]
        spare = pieces[0][0]
        for piece, valid in pieces[1:]:
            spare = jnp.where(some, spare, piece)
            some = jnp.logical_or(some, valid)

        @pl.when(some)
        def _():
            keys, values = [], []
            for piece, valid in pieces:
                at = jnp.where(valid, piece, spare)
                weight = jnp.full((PIECE, WIDTH), jnp.where(valid, 1.0, 0.0), jnp.float32).astype(jnp.bfloat16)
                keys.append(buf[at, :, :WIDTH])
                values.append(jnp.concatenate([buf[at, :, WIDTH:] * weight, weight], axis=1))
            s = scores_of(jnp.concatenate(keys, axis=0))
            parts = [s[:, at * WIDTH : (at + 1) * WIDTH] for at in range(len(pieces))]
            old = top[...]
            new = jnp.maximum(old, row_max(parts))
            top[...] = new
            shrink = jnp.exp2(old - new)
            p = jnp.concatenate([jnp.exp2(part - new).astype(jnp.bfloat16) for part in parts], axis=1)
            fresh = jnp.dot(p, jnp.concatenate(values, axis=0), preferred_element_type=jnp.float32)
            acc[:, :WIDTH] = acc[:, :WIDTH] * shrink + fresh[:, :WIDTH]
            acc[:, WIDTH:] = acc[:, WIDTH:] * shrink + fresh[:, WIDTH:]

    def step(n, carry):
        now = jnp.minimum(n, EVENTS - 1)
        live = n < EVENTS
        j, k, kl, kr = decode(now)
        left = cell_at(my_a + offset_of(kl), my_b - j)
        right = cell_at(my_a + offset_of(kr), my_b + j)
        both = kr < 8

        @pl.when(jnp.logical_and(live, j == 0))
        def _():
            wait_own(left)

            @pl.when(k < 4)
            def _():
                pass_on(left, a_up)

            pass_on(left, b_up)
            pass_on(left, b_down)
            share(left)

            @pl.when(k < 4)
            def _():
                wait_own(right)

                @pl.when(k < 3)
                def _():
                    pass_on(right, a_down)

                pass_on(right, b_up)
                pass_on(right, b_down)
                share(right)

        @pl.when(jnp.logical_and(live, j > 0))
        def _():
            wait_own(left)

            @pl.when(jnp.logical_or(j < 3, jnp.logical_and(j == 3, kl % 2 == (kl // 2) % 2)))
            def _():
                pass_on(left, b_up)

            share(left)
            wait_own(right)

            @pl.when(jnp.logical_or(j < 3, jnp.logical_and(j == 3, kr % 2 != (kr // 2) % 2)))
            def _():
                pass_on(right, b_down)

            share(right)

        past = jnp.maximum(n - LAG, 0)
        due = n >= LAG
        j2, k2, kl2, kr2 = decode(past)
        left2 = other_cell_at(my_b + offset_of(kl2), my_a - j2)
        right2 = other_cell_at(my_b + offset_of(kr2), my_a + j2)
        both2 = kr2 < 8

        @pl.when(due)
        def _():
            wait_other(left2)

            @pl.when(both2)
            def _():
                wait_other(right2)

        attend(
            [
                (mine + left, jnp.logical_and(live, left < cell)),
                (mine + right, jnp.logical_and(jnp.logical_and(live, both), right < cell)),
                (theirs + left2, jnp.logical_and(due, left2 < cell)),
                (theirs + right2, jnp.logical_and(jnp.logical_and(due, both2), right2 < cell)),
            ]
        )
        return carry

    lax.fori_loop(0, EVENTS + LAG, step, 0)

    o = (acc[:, :WIDTH] / acc[:, WIDTH:]).astype(jnp.bfloat16)
    obuf[...] = o.reshape(GROUP, 2, 2, HALF // 2, WIDTH)
    heads = pl.ds(pl.multiple_of(tp * 8 + xh * 4, 4), GROUP)
    places = ((xh, 1 - tp, side), (1 - xh, tp, swap), (1 - xh, 1 - tp, cross))
    for at, (to_xh, to_tp, device) in enumerate(places):
        remote(obuf.at[:, to_xh, to_tp], out_ref.at[heads], out_send.at[at], out_recv.at[at], device).start()
    out_ref[heads] = obuf[:, xh, tp]
    for at, (to_xh, to_tp, device) in enumerate(places):
        from_heads = pl.ds(pl.multiple_of(to_tp * 8 + to_xh * 4, 4), GROUP)
        remote(obuf.at[:, to_xh, to_tp], out_ref.at[from_heads], out_send.at[at], out_recv.at[at], device).wait()

    kv_out.wait_send()
    q_out.wait_send()
    everything = buf.at[pl.ds(0, 127)]
    remote(everything, everything, send_sem, own_sem.at[cell], b_up).wait_send()


def per_device(queries, incoming_lookup_vectors, incoming_content_vectors):
    tok_rows = queries.shape[0]
    my_index = lax.axis_index("ctx")
    natural_pos = my_index * tok_rows + jnp.arange(tok_rows, dtype=jnp.int32)
    key_cache = rotate(incoming_lookup_vectors, natural_pos)
    spun = rotate(queries, natural_pos).transpose(1, 0, 2)
    pair = jnp.concatenate([key_cache, incoming_content_vectors], axis=-1).transpose(1, 0, 2)
    vmem = pl.BlockSpec(memory_space=pltpu.VMEM)
    out = pl.pallas_call(
        kernel,
        out_shape=jax.ShapeDtypeStruct((16, HALF // 2, WIDTH), jnp.bfloat16),
        in_specs=[vmem, vmem],
        out_specs=vmem,
        scratch_shapes=[
            pltpu.VMEM((2 * CELLS, PIECE, 2 * WIDTH), jnp.bfloat16),
            pltpu.VMEM((GROUP, 2, HALF, WIDTH), jnp.bfloat16),
            pltpu.VMEM((GROUP, 2, 2, HALF // 2, WIDTH), jnp.bfloat16),
            pltpu.VMEM((ROWS, 2 * WIDTH), jnp.float32),
            pltpu.VMEM((ROWS, WIDTH), jnp.float32),
            pltpu.SemaphoreType.DMA,
            pltpu.SemaphoreType.DMA((CELLS,)),
            pltpu.SemaphoreType.DMA((CELLS,)),
            pltpu.SemaphoreType.DMA((2,)),
            pltpu.SemaphoreType.DMA((2,)),
            pltpu.SemaphoreType.DMA((3,)),
            pltpu.SemaphoreType.DMA((3,)),
        ],
        compiler_params=pltpu.CompilerParams(
            collective_id=0, has_side_effects=True, vmem_limit_bytes=48 * 1024 * 1024
        ),
        name="cell_attention",
    )(spun, pair)
    return (out.transpose(1, 0, 2), key_cache)


def solution(mesh):
    return jax.shard_map(
        per_device,
        mesh=mesh,
        in_specs=(P("ctx", "tp", None), P("ctx", "tp", None), P("ctx", "tp", None)),
        out_specs=(P(("ctx", "tp"), None, None), P("ctx", "tp", None)),
        check_vma=False,
    )
```

```python
import functools
import math

import jax
import jax.numpy as jnp
from jax import lax
from jax.experimental import pallas as pl
from jax.experimental.pallas import tpu as pltpu
from jax.sharding import PartitionSpec as P

MESH = pl.DeviceIdType.MESH
rope_base = 500000.0
RING = 8
CELLS = RING * RING
HALF = 64
PIECE = 2 * HALF
WIDTH = 128
GROUP = 4
ROWS = GROUP * PIECE
BATCH = 2


def rotate(tensor, positions):
    feature_width = tensor.shape[-1]
    half_width = feature_width // 2
    inverse_freq = rope_base ** (-(jnp.arange(half_width, dtype=jnp.float32) * 2.0 / feature_width))
    angles = positions.astype(jnp.float32)[:, None] * inverse_freq[None, :]
    cosine = jnp.cos(angles)[:, None, :]
    sine_part = jnp.sin(angles)[:, None, :]
    widened = tensor.astype(jnp.float32)
    front_half = widened[..., :half_width]
    second = widened[..., half_width:]
    return jnp.concatenate(
        [front_half * cosine - second * sine_part, second * cosine + front_half * sine_part],
        axis=-1,
    ).astype(jnp.bfloat16)


def offset_of(k):
    return ((k + 1) // 2) * (1 - 2 * (k % 2))


def far_left(k):
    return 4 if k in (0, 3, 4, 7) else 3


def far_right(k):
    return 7 - far_left(k)


def event_order():
    entries = [(i, 0, 2 * i - 1, 2 * i if i < 4 else None) for i in range(1, 5)]
    for j in range(1, 4):
        for k in range(8):
            entries.append((j + abs(offset_of(k)), j, k, k))
    for left, right in ((0, 1), (3, 2), (4, 5), (7, 6)):
        entries.append((4 + max(abs(offset_of(left)), abs(offset_of(right))), 4, left, right))
    entries.sort(key=lambda e: e[:3])
    return [e[1:] for e in entries]


ORDER = event_order()
SENDS = 8 * len(ORDER)


def kernel(q_ref, kv_ref, out_ref, buf, qbuf, obuf, acc, top, first_send, send_sem, own_sem, other_sem, swap_send, swap_recv, out_send, out_recv):
    ctx = lax.axis_index("ctx")
    tp = lax.axis_index("tp")
    core = ctx % 2
    xh = (ctx // 2) % 2
    cell = ctx // 4
    y = cell % RING
    z = cell // RING
    zfirst = core == 0

    def pick(flag, one, two):
        return jnp.where(flag, jnp.int32(one), jnp.int32(two))

    def pick_flag(flag, one, two):
        return pick(flag, one, two) != 0

    def cell_at(dz, dy):
        return ((z + dz + RING) % RING) * RING + (y + dy + RING) % RING

    def dev(at):
        return (at * 4 + xh * 2 + core, tp)

    steps = pick(zfirst, 1, 0)
    a_up = dev(cell_at(steps, 1 - steps))
    a_down = dev(cell_at(-steps, steps - 1))
    b_up = dev(cell_at(1 - steps, steps))
    b_down = dev(cell_at(steps - 1, -steps))
    mate = (cell * 4 + xh * 2 + 1 - core, tp)
    swap = (cell * 4 + (1 - xh) * 2 + core, tp)
    side = (ctx, 1 - tp)
    cross = (cell * 4 + (1 - xh) * 2 + core, 1 - tp)

    barrier = pltpu.get_barrier_semaphore()
    for device in (a_up, a_down, b_up, b_down, mate, swap, side, cross):
        pl.semaphore_signal(barrier, inc=1, device_id=device, device_id_type=MESH)
    pl.semaphore_wait(barrier, 8)

    mine = core * CELLS
    theirs = (1 - core) * CELLS
    own = mine + cell
    keep_rows = pl.ds(pl.multiple_of(xh * HALF, HALF), HALF)
    get_rows = pl.ds(pl.multiple_of((1 - xh) * HALF, HALF), HALF)

    def remote(src, dst, s_sem, r_sem, device):
        return pltpu.make_async_remote_copy(
            src_ref=src, dst_ref=dst, send_sem=s_sem, recv_sem=r_sem, device_id=device, device_id_type=MESH
        )

    kv_out = remote(kv_ref.at[1 - xh], buf.at[own, keep_rows], swap_send.at[0], swap_recv.at[0], swap)
    kv_out.start()
    below_top = z < RING - 1
    low = z < 3
    first_targets = (
        (a_up, pick_flag(zfirst, below_top, True)),
        (a_down, pick_flag(zfirst, low, True)),
        (b_up, pick_flag(zfirst, True, below_top)),
        (b_down, pick_flag(zfirst, True, low)),
    )

    def first_copies(src, part):
        for at, (device, needed) in enumerate(first_targets):
            yield needed, remote(src, buf.at[own, part], first_send.at[at], own_sem.at[cell], device)
        yield None, remote(src, buf.at[own, part], first_send.at[4], other_sem.at[cell], mate)

    def start_first(src, part):
        for needed, copy in first_copies(src, part):
            if needed is None:
                copy.start()
            else:
                pl.when(needed)(copy.start)

    start_first(kv_ref.at[xh], keep_rows)
    other_heads = pl.ds(pl.multiple_of((1 - xh) * GROUP, GROUP), GROUP)
    own_heads = pl.ds(pl.multiple_of(xh * GROUP, GROUP), GROUP)
    q_out = remote(q_ref.at[other_heads], qbuf.at[:, xh], swap_send.at[1], swap_recv.at[1], swap)
    q_out.start()
    buf[own, keep_rows] = kv_ref[xh]
    qbuf[:, xh] = q_ref[own_heads]

    remote(kv_ref.at[1 - xh], buf.at[own, get_rows], swap_send.at[0], swap_recv.at[0], swap).wait_recv()
    start_first(buf.at[own, get_rows], get_rows)
    remote(q_ref.at[other_heads], qbuf.at[:, 1 - xh], swap_send.at[1], swap_recv.at[1], swap).wait_recv()

    def piece_of(event, right, first_z):
        j, kl, kr = event
        k = kr if right else kl
        if k is None:
            return None
        along = offset_of(k)
        across = j if right else -j
        zz = (z + pick(first_z, along, across) + RING) % RING
        yy = (y + pick(first_z, across, along) + RING) % RING
        at = zz * RING + yy
        if j == 0:
            comes = pick_flag(first_z, zz < (3 if right else z), True)
        else:
            comes = pick_flag(first_z, zz <= z, zz < (far_right(k) if right else z))
        return at, comes, at < cell, zz

    def routes(event, right):
        j, kl, kr = event
        k = kr if right else kl
        zz = piece_of(event, right, zfirst)[3]
        if j == 0:
            ring_end = k >= (5 if right else 7)
            if not ring_end:
                yield (a_down if right else a_up), pick_flag(zfirst, True if right else below_top, True)
            yield b_up, pick_flag(zfirst, zz < z, below_top)
            yield b_down, pick_flag(zfirst, zz < z, z < far_right(k))
        elif right:
            if j < far_right(k):
                yield b_down, None
        elif j < far_left(k):
            yield b_up, pick_flag(zfirst, True, below_top)

    def copies(n, right):
        event = ORDER[n]
        at, _, seen, _ = piece_of(event, right, zfirst)
        spot = buf.at[mine + at]
        base = n * 8 + (4 if right else 0)
        yield seen, remote(spot, spot, send_sem.at[base], other_sem.at[at], mate)
        for place, (device, needed) in enumerate(routes(event, right)):
            yield needed, remote(spot, spot, send_sem.at[base + 1 + place], own_sem.at[at], device)

    def each_side(n, act):
        for right in (False, True):
            found = piece_of(ORDER[n], right, zfirst)
            if found is None:
                continue

            @pl.when(found[1])
            def _():
                act(n, right, found[0])

    def take(n, right, at):
        spot = buf.at[mine + at]
        remote(spot, spot, send_sem.at[0], own_sem.at[at], b_up).wait_recv()
        for needed, copy in copies(n, right):
            if needed is None:
                copy.start()
            else:
                pl.when(needed)(copy.start)

    def finish(n, right, at):
        for needed, copy in copies(n, right):
            if needed is None:
                copy.wait_send()
            else:
                pl.when(needed)(copy.wait_send)

    def wait_other(at):
        spot = buf.at[theirs + at]
        remote(spot, spot, send_sem.at[0], other_sem.at[at], mate).wait_recv()

    factor = math.log2(math.e) / math.sqrt(WIDTH)

    def scores_of(keys):
        q = qbuf[...].reshape(ROWS, WIDTH)
        return lax.dot_general(keys, q, (((1,), (1,)), ((), ())), preferred_element_type=jnp.float32)

    def weigh(values, p):
        return lax.dot_general(
            values, p.astype(jnp.bfloat16), (((0,), (0,)), ((), ())), preferred_element_type=jnp.float32
        )

    wait_other(cell)
    key = lax.broadcasted_iota(jnp.int32, (PIECE, ROWS), 0)
    row = lax.broadcasted_iota(jnp.int32, (PIECE, ROWS), 1) % PIECE
    row_at = jnp.where(row < HALF, row, row + HALF) + core * HALF
    key_at = jnp.where(key < HALF, key, key + HALF)
    both = (own, theirs + cell)
    s = scores_of(jnp.concatenate([buf[piece, :, :WIDTH] for piece in both], axis=0))
    s = jnp.concatenate(
        [
            jnp.where(row_at >= key_at + core * HALF, s[:PIECE], -1e30),
            jnp.where(row_at >= key_at + (1 - core) * HALF, s[PIECE:], -1e30),
        ],
        axis=0,
    )
    most = jnp.max(s, axis=0, keepdims=True)
    top[0:1] = most
    p = jnp.exp2((s - most) * factor)
    acc[WIDTH : WIDTH + 1] = jnp.sum(p, axis=0, keepdims=True)
    acc[:WIDTH] = weigh(jnp.concatenate([buf[piece, :, WIDTH:] for piece in both], axis=0), p)

    def attend(pieces):
        some = pieces[0][1]
        for _, seen in pieces[1:]:
            some = jnp.logical_or(some, seen)

        @pl.when(some)
        def _():
            spots = [jnp.where(seen, piece, own) for piece, seen in pieces]
            hide = [jnp.where(seen, 0.0, 1e30) for _, seen in pieces]
            s = scores_of(jnp.concatenate([buf[at, :, :WIDTH] for at in spots], axis=0))
            parts = [s[at * PIECE : (at + 1) * PIECE] for at in range(len(pieces))]
            old = top[0:1]
            new = old
            for part, away in zip(parts, hide):
                new = jnp.maximum(new, jnp.max(part, axis=0, keepdims=True) - away)
            top[0:1] = new
            shrink = jnp.exp2((old - new) * factor)
            p = jnp.concatenate([jnp.exp2((part - (new + away)) * factor) for part, away in zip(parts, hide)], axis=0)
            fresh = weigh(jnp.concatenate([buf[at, :, WIDTH:] for at in spots], axis=0), p)
            acc[WIDTH : WIDTH + 1] = acc[WIDTH : WIDTH + 1] * shrink + jnp.sum(p, axis=0, keepdims=True)
            acc[:WIDTH] = acc[:WIDTH] * shrink + fresh

    events = len(ORDER)
    for start in range(0, events + BATCH, BATCH):
        pieces = []
        for n in range(start, start + BATCH):
            if n < events:
                each_side(n, take)
                for right in (False, True):
                    found = piece_of(ORDER[n], right, zfirst)
                    if found is not None:
                        pieces.append((mine + found[0], found[2]))
        for n in range(start - BATCH, start):
            if n >= 0:
                for right in (False, True):
                    found = piece_of(ORDER[n], right, jnp.logical_not(zfirst))
                    if found is not None:
                        pl.when(found[2])(functools.partial(wait_other, found[0]))
                        pieces.append((theirs + found[0], found[2]))
        attend(pieces)

    o = (acc[:WIDTH] / acc[WIDTH : WIDTH + 1]).T.astype(jnp.bfloat16)
    obuf[...] = o.reshape(GROUP, 2, 2, HALF // 2, WIDTH)
    heads = pl.ds(pl.multiple_of(tp * 8 + xh * 4, 4), GROUP)
    places = ((xh, 1 - tp, side), (1 - xh, tp, swap), (1 - xh, 1 - tp, cross))
    for at, (to_xh, to_tp, device) in enumerate(places):
        remote(obuf.at[:, to_xh, to_tp], out_ref.at[heads], out_send.at[at], out_recv.at[at], device).start()
    out_ref[heads] = obuf[:, xh, tp]
    kv_out.wait_send()
    q_out.wait_send()
    whole = buf.at[own]
    for at, (device, needed) in enumerate(first_targets):
        pl.when(needed)(remote(whole, whole, first_send.at[at], own_sem.at[cell], device).wait_send)
    remote(whole, whole, first_send.at[4], other_sem.at[cell], mate).wait_send()
    for n in range(events):
        each_side(n, finish)
    for at, (to_xh, to_tp, device) in enumerate(places):
        from_heads = pl.ds(pl.multiple_of(to_tp * 8 + to_xh * 4, 4), GROUP)
        remote(obuf.at[:, to_xh, to_tp], out_ref.at[from_heads], out_send.at[at], out_recv.at[at], device).wait()


def per_device(queries, incoming_lookup_vectors, incoming_content_vectors):
    tok_rows = queries.shape[0]
    my_index = lax.axis_index("ctx")
    natural_pos = my_index * tok_rows + jnp.arange(tok_rows, dtype=jnp.int32)
    key_cache = rotate(incoming_lookup_vectors, natural_pos)
    spun = rotate(queries, natural_pos).transpose(1, 0, 2)
    pair = jnp.concatenate([key_cache, incoming_content_vectors], axis=-1).transpose(1, 0, 2)
    vmem = pl.BlockSpec(memory_space=pltpu.VMEM)
    out = pl.pallas_call(
        kernel,
        out_shape=jax.ShapeDtypeStruct((16, HALF // 2, WIDTH), jnp.bfloat16),
        in_specs=[vmem, vmem],
        out_specs=vmem,
        scratch_shapes=[
            pltpu.VMEM((2 * CELLS, PIECE, 2 * WIDTH), jnp.bfloat16),
            pltpu.VMEM((GROUP, 2, HALF, WIDTH), jnp.bfloat16),
            pltpu.VMEM((GROUP, 2, 2, HALF // 2, WIDTH), jnp.bfloat16),
            pltpu.VMEM((WIDTH + 8, ROWS), jnp.float32),
            pltpu.VMEM((8, ROWS), jnp.float32),
            pltpu.SemaphoreType.DMA((5,)),
            pltpu.SemaphoreType.DMA((SENDS,)),
            pltpu.SemaphoreType.DMA((CELLS,)),
            pltpu.SemaphoreType.DMA((CELLS,)),
            pltpu.SemaphoreType.DMA((2,)),
            pltpu.SemaphoreType.DMA((2,)),
            pltpu.SemaphoreType.DMA((3,)),
            pltpu.SemaphoreType.DMA((3,)),
        ],
        compiler_params=pltpu.CompilerParams(
            collective_id=0, has_side_effects=True, vmem_limit_bytes=48 * 1024 * 1024
        ),
        name="cell_attention",
    )(spun, pair)
    return (out.transpose(1, 0, 2), key_cache)


def solution(mesh):
    return jax.shard_map(
        per_device,
        mesh=mesh,
        in_specs=(P("ctx", "tp", None), P("ctx", "tp", None), P("ctx", "tp", None)),
        out_specs=(P(("ctx", "tp"), None, None), P("ctx", "tp", None)),
        check_vma=False,
    )
```

```python
import functools
import math

import jax
import jax.numpy as jnp
from jax import lax
from jax.experimental import pallas as pl
from jax.experimental.pallas import tpu as pltpu
from jax.sharding import PartitionSpec as P

MESH = pl.DeviceIdType.MESH
rope_base = 500000.0
RING = 8
CELLS = RING * RING
HALF = 64
PIECE = 2 * HALF
WIDTH = 128
GROUP = 4
ROWS = GROUP * PIECE
BATCH = 2


def offset_of(k):
    return ((k + 1) // 2) * (1 - 2 * (k % 2))


def far_left(k):
    return 4 if k in (0, 3, 4, 7) else 3


def far_right(k):
    return 7 - far_left(k)


def event_order():
    entries = [(i, 0, 2 * i - 1, 2 * i if i < 4 else None) for i in range(1, 5)]
    for j in range(1, 4):
        for k in range(8):
            entries.append((j + abs(offset_of(k)), j, k, k))
    for left, right in ((0, 1), (3, 2), (4, 5), (7, 6)):
        entries.append((4 + max(abs(offset_of(left)), abs(offset_of(right))), 4, left, right))
    entries.sort(key=lambda e: e[:3])
    return [e[1:] for e in entries]


ORDER = event_order()
EVENTS = len(ORDER)
BATCHES = EVENTS // BATCH


def landing_events():
    found = {}
    for n, (j, kl, kr) in enumerate(ORDER):
        found[j, False, kl] = n
        if kr is not None:
            found[j, True, kr] = n
    return found


LANDING = landing_events()


def sends_of(first_z, z, y):
    top_row, low = z == RING - 1, z < 3
    total = 1 + (not (first_z and top_row)) + (not first_z or low) + (first_z or not top_row) + (first_z or low)
    for j, kl, kr in ORDER:
        for right, k in ((False, kl), (True, kr)):
            if k is None:
                continue
            along, across = offset_of(k), j if right else -j
            zz = (z + (along if first_z else across)) % RING
            yy = (y + (across if first_z else along)) % RING
            if j == 0:
                comes = zz < (3 if right else z) if first_z else True
            else:
                comes = zz <= z if first_z else zz < (far_right(k) if right else z)
            if not comes:
                continue
            total += zz * RING + yy < z * RING + y
            if j == 0:
                if k < (5 if right else 7):
                    total += not (first_z and not right and top_row)
                total += zz < z if first_z else not top_row
                total += zz < z if first_z else z < far_right(k)
            elif right:
                total += j < far_right(k)
            elif j < far_left(k):
                total += first_z or not top_row
    return total


TOTALS = sorted({sends_of(f, z, y) for f in (True, False) for z in range(RING) for y in range(RING)})


def kernel(q_raw, k_raw, v_raw, cos_ref, sin_ref, out_ref, key_ref, q_ref, kv_ref, landed, buf, qbuf, obuf, acc, top, send_sem, own_sem, other_sem, swap_send, swap_recv, out_send, out_recv):
    ctx = lax.axis_index("ctx")
    tp = lax.axis_index("tp")
    core = ctx % 2
    xh = (ctx // 2) % 2
    cell = ctx // 4
    y = cell % RING
    z = cell // RING
    zfirst = core == 0

    def pick(flag, one, two):
        return jnp.where(flag, jnp.int32(one), jnp.int32(two))

    def pick_flag(flag, one, two):
        return pick(flag, one, two) != 0

    def cell_at(dz, dy):
        return ((z + dz + RING) % RING) * RING + (y + dy + RING) % RING

    def dev(at):
        return (at * 4 + xh * 2 + core, tp)

    steps = pick(zfirst, 1, 0)
    a_up = dev(cell_at(steps, 1 - steps))
    a_down = dev(cell_at(-steps, steps - 1))
    b_up = dev(cell_at(1 - steps, steps))
    b_down = dev(cell_at(steps - 1, -steps))
    mate = (cell * 4 + xh * 2 + 1 - core, tp)
    swap = (cell * 4 + (1 - xh) * 2 + core, tp)
    side = (ctx, 1 - tp)
    cross = (cell * 4 + (1 - xh) * 2 + core, 1 - tp)

    barrier = pltpu.get_barrier_semaphore()
    for device in (a_up, a_down, b_up, b_down, mate, swap, side, cross):
        pl.semaphore_signal(barrier, inc=1, device_id=device, device_id_type=MESH)

    cosine = cos_ref[...][:, None, :]
    sine = sin_ref[...][:, None, :]

    def rotated(raw):
        wide = raw[...].astype(jnp.float32)
        return wide * cosine + pltpu.roll(wide, WIDTH // 2, 2) * sine

    keys = rotated(k_raw)
    key_ref[...] = keys.astype(jnp.bfloat16)
    kv_ref[:, :, :WIDTH] = jnp.swapaxes(keys, 0, 1).astype(jnp.bfloat16)
    kv_ref[:, :, WIDTH:] = jnp.swapaxes(v_raw[...].astype(jnp.float32), 0, 1).astype(jnp.bfloat16)
    q_ref[...] = jnp.swapaxes(rotated(q_raw), 0, 1).astype(jnp.bfloat16)

    pl.semaphore_wait(barrier, 8)

    mine = core * CELLS
    theirs = (1 - core) * CELLS
    own = mine + cell
    keep_rows = pl.ds(pl.multiple_of(xh * HALF, HALF), HALF)
    get_rows = pl.ds(pl.multiple_of((1 - xh) * HALF, HALF), HALF)

    def remote(src, dst, s_sem, r_sem, device):
        return pltpu.make_async_remote_copy(
            src_ref=src, dst_ref=dst, send_sem=s_sem, recv_sem=r_sem, device_id=device, device_id_type=MESH
        )

    kv_out = remote(kv_ref.at[1 - xh], buf.at[own, keep_rows], swap_send.at[0], swap_recv.at[0], swap)
    kv_out.start()
    below_top = z < RING - 1
    low = z < 3
    first_targets = (
        (a_up, pick_flag(zfirst, below_top, True)),
        (a_down, pick_flag(zfirst, low, True)),
        (b_up, pick_flag(zfirst, True, below_top)),
        (b_down, pick_flag(zfirst, True, low)),
    )

    first_sems = (LANDING[0, False, 1], LANDING[0, True, 2], LANDING[1, False, 0], LANDING[1, True, 0])
    sent = [jnp.int32(1)] + [needed.astype(jnp.int32) for _, needed in first_targets]

    def start_first(src, part):
        for at, (device, needed) in zip(first_sems, first_targets):
            pl.when(needed)(remote(src, buf.at[own, part], send_sem, own_sem.at[at], device).start)
        remote(src, buf.at[own, part], send_sem, other_sem.at[BATCHES], mate).start()

    start_first(kv_ref.at[xh], keep_rows)
    other_heads = pl.ds(pl.multiple_of((1 - xh) * GROUP, GROUP), GROUP)
    own_heads = pl.ds(pl.multiple_of(xh * GROUP, GROUP), GROUP)
    q_out = remote(q_ref.at[other_heads], qbuf.at[:, xh], swap_send.at[1], swap_recv.at[1], swap)
    q_out.start()
    buf[own, keep_rows] = kv_ref[xh]
    qbuf[:, xh] = q_ref[own_heads]

    remote(kv_ref.at[1 - xh], buf.at[own, get_rows], swap_send.at[0], swap_recv.at[0], swap).wait_recv()
    start_first(buf.at[own, get_rows], get_rows)
    remote(q_ref.at[other_heads], qbuf.at[:, 1 - xh], swap_send.at[1], swap_recv.at[1], swap).wait_recv()

    def piece_of(event, right, first_z):
        j, kl, kr = event
        k = kr if right else kl
        if k is None:
            return None
        along = offset_of(k)
        across = j if right else -j
        zz = (z + pick(first_z, along, across) + RING) % RING
        yy = (y + pick(first_z, across, along) + RING) % RING
        at = zz * RING + yy
        if j == 0:
            comes = pick_flag(first_z, zz < (3 if right else z), True)
        else:
            comes = pick_flag(first_z, zz <= z, zz < (far_right(k) if right else z))
        return at, comes, at < cell, zz

    def routes(event, right):
        j, kl, kr = event
        k = kr if right else kl
        zz = piece_of(event, right, zfirst)[3]
        if j == 0:
            ring_end = k >= (5 if right else 7)
            if not ring_end:
                going = pick_flag(zfirst, True if right else below_top, True)
                yield (a_down if right else a_up), going, LANDING[0, right, k + 2]
            yield b_up, pick_flag(zfirst, zz < z, below_top), LANDING[1, False, k]
            yield b_down, pick_flag(zfirst, zz < z, z < far_right(k)), LANDING[1, True, k]
        elif right:
            if j < far_right(k):
                yield b_down, True, LANDING[j + 1, True, k]
        elif j < far_left(k):
            yield b_up, pick_flag(zfirst, True, below_top), LANDING[j + 1, False, k]

    def take(n):
        sides = []
        for right in (False, True):
            found = piece_of(ORDER[n], right, zfirst)
            if found is not None:
                sides.append((right,) + found)
        count = sum(comes.astype(jnp.int32) for _, _, comes, _, _ in sides)
        for many in range(1, len(sides) + 1):
            spots = buf.at[pl.ds(0, many)]
            pl.when(count == many)(remote(spots, spots, send_sem, own_sem.at[n], b_up).wait_recv)
        for right, at, comes, seen, _ in sides:
            spot = buf.at[mine + at]
            ways = [(mate, seen, other_sem.at[n // BATCH])]
            ways += [(device, needed, own_sem.at[land]) for device, needed, land in routes(ORDER[n], right)]
            for device, needed, sem in ways:
                needed = jnp.logical_and(comes, needed)
                sent.append(needed.astype(jnp.int32))
                pl.when(needed)(remote(spot, spot, send_sem, sem, device).start)

    def wait_other(batch, seen):
        count = sum(flag.astype(jnp.int32) for flag in seen)
        for many in range(1, len(seen) + 1):
            spots = buf.at[pl.ds(0, many)]
            pl.when(count == many)(remote(spots, spots, send_sem, other_sem.at[batch], mate).wait_recv)

    factor = math.log2(math.e) / math.sqrt(WIDTH)

    def scores_of(keys):
        q = qbuf[...].reshape(ROWS, WIDTH)
        return lax.dot_general(keys, q, (((1,), (1,)), ((), ())), preferred_element_type=jnp.float32)

    def weigh(values, p):
        return lax.dot_general(
            values, p.astype(jnp.bfloat16), (((0,), (0,)), ((), ())), preferred_element_type=jnp.float32
        )

    whole = buf.at[theirs + cell]
    remote(whole, whole, send_sem, other_sem.at[BATCHES], mate).wait_recv()
    key = lax.broadcasted_iota(jnp.int32, (PIECE, ROWS), 0)
    row = lax.broadcasted_iota(jnp.int32, (PIECE, ROWS), 1) % PIECE
    row_at = jnp.where(row < HALF, row, row + HALF) + core * HALF
    key_at = jnp.where(key < HALF, key, key + HALF)
    both = (own, theirs + cell)
    s = scores_of(jnp.concatenate([buf[piece, :, :WIDTH] for piece in both], axis=0))
    s = jnp.concatenate(
        [
            jnp.where(row_at >= key_at + core * HALF, s[:PIECE], -1e30),
            jnp.where(row_at >= key_at + (1 - core) * HALF, s[PIECE:], -1e30),
        ],
        axis=0,
    )
    most = jnp.max(s, axis=0, keepdims=True)
    top[0:1] = most
    p = jnp.exp2((s - most) * factor)
    acc[WIDTH : WIDTH + 1] = jnp.sum(p, axis=0, keepdims=True)
    acc[:WIDTH] = weigh(jnp.concatenate([buf[piece, :, WIDTH:] for piece in both], axis=0), p)

    def attend(pieces):
        some = pieces[0][1]
        for _, seen in pieces[1:]:
            some = jnp.logical_or(some, seen)

        @pl.when(some)
        def _():
            spots = [jnp.where(seen, piece, own) for piece, seen in pieces]
            hide = [jnp.where(seen, 0.0, 1e30) for _, seen in pieces]
            s = scores_of(jnp.concatenate([buf[at, :, :WIDTH] for at in spots], axis=0))
            parts = [s[at * PIECE : (at + 1) * PIECE] for at in range(len(pieces))]
            old = top[0:1]
            new = old
            for part, away in zip(parts, hide):
                new = jnp.maximum(new, jnp.max(part, axis=0, keepdims=True) - away)
            top[0:1] = new
            shrink = jnp.exp2((old - new) * factor)
            p = jnp.concatenate([jnp.exp2((part - (new + away)) * factor) for part, away in zip(parts, hide)], axis=0)
            fresh = weigh(jnp.concatenate([buf[at, :, WIDTH:] for at in spots], axis=0), p)
            acc[WIDTH : WIDTH + 1] = acc[WIDTH : WIDTH + 1] * shrink + jnp.sum(p, axis=0, keepdims=True)
            acc[:WIDTH] = acc[:WIDTH] * shrink + fresh

    for start in range(0, EVENTS + BATCH, BATCH):
        pieces = []
        for n in range(start, min(start + BATCH, EVENTS)):
            take(n)
            for right in (False, True):
                found = piece_of(ORDER[n], right, zfirst)
                if found is not None:
                    pieces.append((mine + found[0], found[2]))
        if start > 0:
            theirs_now = []
            for n in range(start - BATCH, start):
                for right in (False, True):
                    found = piece_of(ORDER[n], right, jnp.logical_not(zfirst))
                    if found is not None:
                        theirs_now.append((theirs + found[0], found[2]))
            wait_other(start // BATCH - 1, [seen for _, seen in theirs_now])
            pieces += theirs_now
        attend(pieces)

    o = (acc[:WIDTH] / acc[WIDTH : WIDTH + 1]).T.astype(jnp.bfloat16)
    obuf[...] = o.reshape(GROUP, 2, 2, HALF // 2, WIDTH)
    heads = pl.ds(pl.multiple_of(tp * 8 + xh * 4, 4), GROUP)
    places = ((xh, 1 - tp, side), (1 - xh, tp, swap), (1 - xh, 1 - tp, cross))
    for at, (to_xh, to_tp, device) in enumerate(places):
        remote(obuf.at[:, to_xh, to_tp], landed.at[heads], out_send.at[at], out_recv.at[at], device).start()
    landed[heads] = obuf[:, xh, tp]
    kv_out.wait_send()
    q_out.wait_send()
    total = sum(sent)
    for many in TOTALS:
        spots = buf.at[pl.ds(0, many)]
        pl.when(total == many)(remote(spots, spots, send_sem, own_sem.at[0], b_up).wait_send)
    for at, (to_xh, to_tp, device) in enumerate(places):
        from_heads = pl.ds(pl.multiple_of(to_tp * 8 + to_xh * 4, 4), GROUP)
        remote(obuf.at[:, to_xh, to_tp], landed.at[from_heads], out_send.at[at], out_recv.at[at], device).wait()
    out_ref[...] = jnp.swapaxes(landed[...].astype(jnp.float32), 0, 1).astype(jnp.bfloat16)


def per_device(queries, incoming_lookup_vectors, incoming_content_vectors):
    tok_rows = queries.shape[0]
    my_index = lax.axis_index("ctx")
    natural_pos = my_index * tok_rows + jnp.arange(tok_rows, dtype=jnp.int32)
    half_width = WIDTH // 2
    inverse_freq = rope_base ** (-(jnp.arange(half_width, dtype=jnp.float32) * 2.0 / WIDTH))
    angles = natural_pos.astype(jnp.float32)[:, None] * inverse_freq[None, :]
    cosine = jnp.cos(angles)
    sine = jnp.sin(angles)
    vmem = pl.BlockSpec(memory_space=pltpu.VMEM)
    return pl.pallas_call(
        kernel,
        out_shape=(
            jax.ShapeDtypeStruct((HALF // 2, 16, WIDTH), jnp.bfloat16),
            jax.ShapeDtypeStruct((HALF, 2, WIDTH), jnp.bfloat16),
        ),
        in_specs=[vmem] * 5,
        out_specs=(vmem, vmem),
        scratch_shapes=[
            pltpu.VMEM((8, HALF, WIDTH), jnp.bfloat16),
            pltpu.VMEM((2, HALF, 2 * WIDTH), jnp.bfloat16),
            pltpu.VMEM((16, HALF // 2, WIDTH), jnp.bfloat16),
            pltpu.VMEM((2 * CELLS, PIECE, 2 * WIDTH), jnp.bfloat16),
            pltpu.VMEM((GROUP, 2, HALF, WIDTH), jnp.bfloat16),
            pltpu.VMEM((GROUP, 2, 2, HALF // 2, WIDTH), jnp.bfloat16),
            pltpu.VMEM((WIDTH + 8, ROWS), jnp.float32),
            pltpu.VMEM((8, ROWS), jnp.float32),
            pltpu.SemaphoreType.DMA,
            pltpu.SemaphoreType.DMA((EVENTS,)),
            pltpu.SemaphoreType.DMA((BATCHES + 1,)),
            pltpu.SemaphoreType.DMA((2,)),
            pltpu.SemaphoreType.DMA((2,)),
            pltpu.SemaphoreType.DMA((3,)),
            pltpu.SemaphoreType.DMA((3,)),
        ],
        compiler_params=pltpu.CompilerParams(
            collective_id=0, has_side_effects=True, vmem_limit_bytes=48 * 1024 * 1024
        ),
        name="cell_attention",
    )(
        queries,
        incoming_lookup_vectors,
        incoming_content_vectors,
        jnp.concatenate([cosine, cosine], axis=1),
        jnp.concatenate([-sine, sine], axis=1),
    )


def solution(mesh):
    return jax.shard_map(
        per_device,
        mesh=mesh,
        in_specs=(P("ctx", "tp", None), P("ctx", "tp", None), P("ctx", "tp", None)),
        out_specs=(P(("ctx", "tp"), None, None), P("ctx", "tp", None)),
        check_vma=False,
    )
```

```python
import functools
import math

import jax
import jax.numpy as jnp
from jax import lax
from jax.experimental import pallas as pl
from jax.experimental.pallas import tpu as pltpu
from jax.sharding import PartitionSpec as P

MESH = pl.DeviceIdType.MESH
rope_base = 500000.0
RING = 8
CELLS = RING * RING
HALF = 64
PIECE = 2 * HALF
WIDTH = 128
GROUP = 4
ROWS = GROUP * PIECE
BATCH = 2


def offset_of(k):
    return ((k + 1) // 2) * (1 - 2 * (k % 2))


def far_left(k):
    return 4 if k in (0, 3, 4, 7) else 3


def far_right(k):
    return 7 - far_left(k)


ORDER = (
    (0, 1, 2), (1, 0, 0), (0, 3, 4), (1, 1, 1), (1, 2, 2), (0, 5, 6), (2, 1, 1), (1, 4, 4),
    (0, 7, None), (1, 3, 3), (1, 5, 5), (1, 6, 6), (2, 4, 4), (2, 2, 2), (1, 7, 7), (2, 3, 3),
    (2, 0, 0), (2, 6, 6), (2, 5, 5), (3, 2, 2), (2, 7, 7), (3, 1, 1), (3, 0, 0), (3, 3, 3),
    (3, 6, 6), (3, 4, 4), (3, 5, 5), (3, 7, 7), (4, 3, 2), (4, 0, 1), (4, 4, 5), (4, 7, 6),
)
EVENTS = len(ORDER)


def schedule():
    groups = [(n, n + 1) for n in range(0, EVENTS - 2, BATCH)] + [(EVENTS - 2,), (EVENTS - 1,)]
    steps = [(groups[0], ())]
    for at in range(1, len(groups) - 1):
        steps.append((groups[at], (at - 1,)))
    last = len(groups) - 1
    steps.append((groups[last], (last - 1, last)))
    return groups, steps


GROUPS, STEPS = schedule()
GROUP_OF = {n: at for at, group in enumerate(GROUPS) for n in group}


def landing_events():
    found = {}
    for n, (j, kl, kr) in enumerate(ORDER):
        found[j, False, kl] = n
        if kr is not None:
            found[j, True, kr] = n
    return found


LANDING = landing_events()


def sends_of(first_z, z, y):
    top_row, low = z == RING - 1, z < 3
    total = 1 + (not (first_z and top_row)) + (not first_z or low) + (first_z or not top_row) + (first_z or low)
    for j, kl, kr in ORDER:
        for right, k in ((False, kl), (True, kr)):
            if k is None:
                continue
            along, across = offset_of(k), j if right else -j
            zz = (z + (along if first_z else across)) % RING
            yy = (y + (across if first_z else along)) % RING
            if j == 0:
                comes = zz < (3 if right else z) if first_z else True
            else:
                comes = zz <= z if first_z else zz < (far_right(k) if right else z)
            if not comes:
                continue
            total += zz * RING + yy < z * RING + y
            if j == 0:
                if k < (5 if right else 7):
                    total += not (first_z and not right and top_row)
                total += zz < z if first_z else not top_row
                total += zz < z if first_z else z < far_right(k)
            elif right:
                total += j < far_right(k)
            elif j < far_left(k):
                total += first_z or not top_row
    return total


TOTALS = sorted({sends_of(f, z, y) for f in (True, False) for z in range(RING) for y in range(RING)})


def kernel(q_raw, k_raw, v_raw, cos_ref, sin_ref, out_ref, key_ref, q_ref, kv_ref, landed, buf, qbuf, obuf, acc, top, send_sem, own_sem, other_sem, swap_send, swap_recv, out_send, out_recv):
    ctx = lax.axis_index("ctx")
    tp = lax.axis_index("tp")
    core = ctx % 2
    xh = (ctx // 2) % 2
    cell = ctx // 4
    y = cell % RING
    z = cell // RING
    zfirst = core == 0

    def pick(flag, one, two):
        return jnp.where(flag, jnp.int32(one), jnp.int32(two))

    def pick_flag(flag, one, two):
        return pick(flag, one, two) != 0

    def cell_at(dz, dy):
        return ((z + dz + RING) % RING) * RING + (y + dy + RING) % RING

    def dev(at):
        return (at * 4 + xh * 2 + core, tp)

    steps = pick(zfirst, 1, 0)
    a_up = dev(cell_at(steps, 1 - steps))
    a_down = dev(cell_at(-steps, steps - 1))
    b_up = dev(cell_at(1 - steps, steps))
    b_down = dev(cell_at(steps - 1, -steps))
    mate = (cell * 4 + xh * 2 + 1 - core, tp)
    swap = (cell * 4 + (1 - xh) * 2 + core, tp)
    side = (ctx, 1 - tp)
    cross = (cell * 4 + (1 - xh) * 2 + core, 1 - tp)

    barrier = pltpu.get_barrier_semaphore()
    for device in (a_up, a_down, b_up, b_down, mate, swap, side, cross):
        pl.semaphore_signal(barrier, inc=1, device_id=device, device_id_type=MESH)

    cosine = cos_ref[...][:, None, :]
    sine = sin_ref[...][:, None, :]

    def rotated(raw):
        wide = raw[...].astype(jnp.float32)
        return wide * cosine + pltpu.roll(wide, WIDTH // 2, 2) * sine

    keys = rotated(k_raw)
    key_ref[...] = keys.astype(jnp.bfloat16)
    kv_ref[:, :, :WIDTH] = jnp.swapaxes(keys, 0, 1).astype(jnp.bfloat16)
    kv_ref[:, :, WIDTH:] = jnp.swapaxes(v_raw[...].astype(jnp.float32), 0, 1).astype(jnp.bfloat16)
    q_ref[...] = jnp.swapaxes(rotated(q_raw), 0, 1).astype(jnp.bfloat16)

    pl.semaphore_wait(barrier, 8)

    mine = core * CELLS
    theirs = (1 - core) * CELLS
    own = mine + cell
    keep_rows = pl.ds(pl.multiple_of(xh * HALF, HALF), HALF)
    get_rows = pl.ds(pl.multiple_of((1 - xh) * HALF, HALF), HALF)

    def remote(src, dst, s_sem, r_sem, device):
        return pltpu.make_async_remote_copy(
            src_ref=src, dst_ref=dst, send_sem=s_sem, recv_sem=r_sem, device_id=device, device_id_type=MESH
        )

    kv_out = remote(kv_ref.at[1 - xh], buf.at[own, keep_rows], swap_send.at[0], swap_recv.at[0], swap)
    kv_out.start()
    below_top = z < RING - 1
    low = z < 3
    first_targets = (
        (a_up, pick_flag(zfirst, below_top, True)),
        (a_down, pick_flag(zfirst, low, True)),
        (b_up, pick_flag(zfirst, True, below_top)),
        (b_down, pick_flag(zfirst, True, low)),
    )

    halves = (keep_rows, get_rows)
    first_sems = (LANDING[0, False, 1], LANDING[0, True, 2], LANDING[1, False, 0], LANDING[1, True, 0])
    sent = [jnp.int32(1)] + [needed.astype(jnp.int32) for _, needed in first_targets]

    def start_first(src, half):
        part = halves[half]
        for at, (device, needed) in zip(first_sems, first_targets):
            pl.when(needed)(remote(src, buf.at[own, part], send_sem, own_sem.at[half, at], device).start)
        remote(src, buf.at[own, part], send_sem, other_sem.at[len(GROUPS)], mate).start()

    start_first(kv_ref.at[xh], 0)
    other_heads = pl.ds(pl.multiple_of((1 - xh) * GROUP, GROUP), GROUP)
    own_heads = pl.ds(pl.multiple_of(xh * GROUP, GROUP), GROUP)
    q_out = remote(q_ref.at[other_heads], qbuf.at[:, xh], swap_send.at[1], swap_recv.at[1], swap)
    q_out.start()
    buf[own, keep_rows] = kv_ref[xh]
    qbuf[:, xh] = q_ref[own_heads]

    def piece_of(event, right, first_z):
        j, kl, kr = event
        k = kr if right else kl
        if k is None:
            return None
        along = offset_of(k)
        across = j if right else -j
        zz = (z + pick(first_z, along, across) + RING) % RING
        yy = (y + pick(first_z, across, along) + RING) % RING
        at = zz * RING + yy
        if j == 0:
            comes = pick_flag(first_z, zz < (3 if right else z), True)
        else:
            comes = pick_flag(first_z, zz <= z, zz < (far_right(k) if right else z))
        return at, comes, at < cell, zz

    def routes(event, right):
        j, kl, kr = event
        k = kr if right else kl
        zz = piece_of(event, right, zfirst)[3]
        if j == 0:
            ring_end = k >= (5 if right else 7)
            if not ring_end:
                going = pick_flag(zfirst, True if right else below_top, True)
                yield (a_down if right else a_up), going, LANDING[0, right, k + 2]
            yield b_up, pick_flag(zfirst, zz < z, below_top), LANDING[1, False, k]
            yield b_down, pick_flag(zfirst, zz < z, z < far_right(k)), LANDING[1, True, k]
        elif right:
            if j < far_right(k):
                yield b_down, True, LANDING[j + 1, True, k]
        elif j < far_left(k):
            yield b_up, pick_flag(zfirst, True, below_top), LANDING[j + 1, False, k]

    def take(n, half):
        sides = []
        for right in (False, True):
            found = piece_of(ORDER[n], right, zfirst)
            if found is not None:
                sides.append((right,) + found)
        count = sum(comes.astype(jnp.int32) for _, _, comes, _, _ in sides)
        for many in range(1, len(sides) + 1):
            spots = buf.at[pl.ds(0, many), pl.ds(0, HALF)]
            pl.when(count == many)(remote(spots, spots, send_sem, own_sem.at[half, n], b_up).wait_recv)
        for right, at, comes, seen, _ in sides:
            spot = buf.at[mine + at, halves[half]]
            for device, needed, land in routes(ORDER[n], right):
                needed = jnp.logical_and(comes, needed)
                pl.when(needed)(remote(spot, spot, send_sem, own_sem.at[half, land], device).start)
                if half:
                    sent.append(needed.astype(jnp.int32))
            if half:
                needed = jnp.logical_and(comes, seen)
                whole = buf.at[mine + at]
                pl.when(needed)(remote(whole, whole, send_sem, other_sem.at[GROUP_OF[n]], mate).start)
                sent.append(needed.astype(jnp.int32))

    def wait_other(batch, seen):
        count = sum(flag.astype(jnp.int32) for flag in seen)
        for many in range(1, len(seen) + 1):
            spots = buf.at[pl.ds(0, many)]
            pl.when(count == many)(remote(spots, spots, send_sem, other_sem.at[batch], mate).wait_recv)

    for n in GROUPS[0]:
        take(n, 0)

    remote(kv_ref.at[1 - xh], buf.at[own, get_rows], swap_send.at[0], swap_recv.at[0], swap).wait_recv()
    start_first(buf.at[own, get_rows], 1)
    remote(q_ref.at[other_heads], qbuf.at[:, 1 - xh], swap_send.at[1], swap_recv.at[1], swap).wait_recv()

    factor = math.log2(math.e) / math.sqrt(WIDTH)

    def scores_of(keys):
        q = qbuf[...].reshape(ROWS, WIDTH)
        return lax.dot_general(keys, q, (((1,), (1,)), ((), ())), preferred_element_type=jnp.float32)

    def weigh(values, p):
        return lax.dot_general(
            values, p.astype(jnp.bfloat16), (((0,), (0,)), ((), ())), preferred_element_type=jnp.float32
        )

    whole = buf.at[theirs + cell]
    remote(whole, whole, send_sem, other_sem.at[len(GROUPS)], mate).wait_recv()
    key = lax.broadcasted_iota(jnp.int32, (PIECE, ROWS), 0)
    row = lax.broadcasted_iota(jnp.int32, (PIECE, ROWS), 1) % PIECE
    row_at = jnp.where(row < HALF, row, row + HALF) + core * HALF
    key_at = jnp.where(key < HALF, key, key + HALF)
    both = (own, theirs + cell)
    s = scores_of(jnp.concatenate([buf[piece, :, :WIDTH] for piece in both], axis=0))
    s = jnp.concatenate(
        [
            jnp.where(row_at >= key_at + core * HALF, s[:PIECE], -1e30),
            jnp.where(row_at >= key_at + (1 - core) * HALF, s[PIECE:], -1e30),
        ],
        axis=0,
    )
    most = jnp.max(s, axis=0, keepdims=True)
    top[0:1] = most
    p = jnp.exp2((s - most) * factor)
    acc[WIDTH : WIDTH + 1] = jnp.sum(p, axis=0, keepdims=True)
    acc[:WIDTH] = weigh(jnp.concatenate([buf[piece, :, WIDTH:] for piece in both], axis=0), p)

    def attend(pieces):
        some = pieces[0][1]
        for _, seen in pieces[1:]:
            some = jnp.logical_or(some, seen)

        @pl.when(some)
        def _():
            spots = [jnp.where(seen, piece, own) for piece, seen in pieces]
            hide = [jnp.where(seen, 0.0, 1e30) for _, seen in pieces]
            s = scores_of(jnp.concatenate([buf[at, :, :WIDTH] for at in spots], axis=0))
            parts = [s[at * PIECE : (at + 1) * PIECE] for at in range(len(pieces))]
            old = top[0:1]
            new = old
            for part, away in zip(parts, hide):
                new = jnp.maximum(new, jnp.max(part, axis=0, keepdims=True) - away)
            top[0:1] = new
            shrink = jnp.exp2((old - new) * factor)
            p = jnp.concatenate([jnp.exp2((part - (new + away)) * factor) for part, away in zip(parts, hide)], axis=0)
            fresh = weigh(jnp.concatenate([buf[at, :, WIDTH:] for at in spots], axis=0), p)
            acc[WIDTH : WIDTH + 1] = acc[WIDTH : WIDTH + 1] * shrink + jnp.sum(p, axis=0, keepdims=True)
            acc[:WIDTH] = acc[:WIDTH] * shrink + fresh

    for fresh_events, shared in STEPS:
        pieces = []
        for half in (0, 1):
            for n in fresh_events:
                if half or n not in GROUPS[0]:
                    take(n, half)
        for n in fresh_events:
            for right in (False, True):
                found = piece_of(ORDER[n], right, zfirst)
                if found is not None:
                    pieces.append((mine + found[0], found[2]))
        for group in shared:
            theirs_now = []
            for n in GROUPS[group]:
                for right in (False, True):
                    found = piece_of(ORDER[n], right, jnp.logical_not(zfirst))
                    if found is not None:
                        theirs_now.append((theirs + found[0], found[2]))
            wait_other(group, [seen for _, seen in theirs_now])
            pieces += theirs_now
        attend(pieces)

    o = (acc[:WIDTH] / acc[WIDTH : WIDTH + 1]).T.astype(jnp.bfloat16)
    obuf[...] = o.reshape(GROUP, 2, 2, HALF // 2, WIDTH)
    heads = pl.ds(pl.multiple_of(tp * 8 + xh * 4, 4), GROUP)
    places = ((xh, 1 - tp, side), (1 - xh, tp, swap), (1 - xh, 1 - tp, cross))
    for at, (to_xh, to_tp, device) in enumerate(places):
        remote(obuf.at[:, to_xh, to_tp], landed.at[heads], out_send.at[at], out_recv.at[at], device).start()
    landed[heads] = obuf[:, xh, tp]
    kv_out.wait_send()
    q_out.wait_send()
    total = sum(sent)
    for many in TOTALS:
        spots = buf.at[pl.ds(0, many)]
        pl.when(total == many)(remote(spots, spots, send_sem, own_sem.at[0, 0], b_up).wait_send)
    for at, (to_xh, to_tp, device) in enumerate(places):
        from_heads = pl.ds(pl.multiple_of(to_tp * 8 + to_xh * 4, 4), GROUP)
        remote(obuf.at[:, to_xh, to_tp], landed.at[from_heads], out_send.at[at], out_recv.at[at], device).wait()
    out_ref[...] = jnp.swapaxes(landed[...].astype(jnp.float32), 0, 1).astype(jnp.bfloat16)


def per_device(queries, incoming_lookup_vectors, incoming_content_vectors):
    tok_rows = queries.shape[0]
    my_index = lax.axis_index("ctx")
    natural_pos = my_index * tok_rows + jnp.arange(tok_rows, dtype=jnp.int32)
    half_width = WIDTH // 2
    inverse_freq = rope_base ** (-(jnp.arange(half_width, dtype=jnp.float32) * 2.0 / WIDTH))
    angles = natural_pos.astype(jnp.float32)[:, None] * inverse_freq[None, :]
    cosine = jnp.cos(angles)
    sine = jnp.sin(angles)
    vmem = pl.BlockSpec(memory_space=pltpu.VMEM)
    return pl.pallas_call(
        kernel,
        out_shape=(
            jax.ShapeDtypeStruct((HALF // 2, 16, WIDTH), jnp.bfloat16),
            jax.ShapeDtypeStruct((HALF, 2, WIDTH), jnp.bfloat16),
        ),
        in_specs=[vmem] * 5,
        out_specs=(vmem, vmem),
        scratch_shapes=[
            pltpu.VMEM((8, HALF, WIDTH), jnp.bfloat16),
            pltpu.VMEM((2, HALF, 2 * WIDTH), jnp.bfloat16),
            pltpu.VMEM((16, HALF // 2, WIDTH), jnp.bfloat16),
            pltpu.VMEM((2 * CELLS, PIECE, 2 * WIDTH), jnp.bfloat16),
            pltpu.VMEM((GROUP, 2, HALF, WIDTH), jnp.bfloat16),
            pltpu.VMEM((GROUP, 2, 2, HALF // 2, WIDTH), jnp.bfloat16),
            pltpu.VMEM((WIDTH + 8, ROWS), jnp.float32),
            pltpu.VMEM((8, ROWS), jnp.float32),
            pltpu.SemaphoreType.DMA,
            pltpu.SemaphoreType.DMA((2, EVENTS)),
            pltpu.SemaphoreType.DMA((len(GROUPS) + 1,)),
            pltpu.SemaphoreType.DMA((2,)),
            pltpu.SemaphoreType.DMA((2,)),
            pltpu.SemaphoreType.DMA((3,)),
            pltpu.SemaphoreType.DMA((3,)),
        ],
        compiler_params=pltpu.CompilerParams(
            collective_id=0, has_side_effects=True, vmem_limit_bytes=48 * 1024 * 1024
        ),
        name="cell_attention",
    )(
        queries,
        incoming_lookup_vectors,
        incoming_content_vectors,
        jnp.concatenate([cosine, cosine], axis=1),
        jnp.concatenate([-sine, sine], axis=1),
    )


def solution(mesh):
    return jax.shard_map(
        per_device,
        mesh=mesh,
        in_specs=(P("ctx", "tp", None), P("ctx", "tp", None), P("ctx", "tp", None)),
        out_specs=(P(("ctx", "tp"), None, None), P("ctx", "tp", None)),
        check_vma=False,
    )
```

```python
import functools
import math

import jax
import jax.numpy as jnp
from jax import lax
from jax.experimental import pallas as pl
from jax.experimental.pallas import tpu as pltpu
from jax.sharding import PartitionSpec as P

MESH = pl.DeviceIdType.MESH
rope_base = 500000.0
RING = 8
CELLS = RING * RING
HALF = 64
PIECE = 2 * HALF
WIDTH = 128
GROUP = 4
ROWS = GROUP * PIECE
BATCH = 2


def offset_of(k):
    return ((k + 1) // 2) * (1 - 2 * (k % 2))


def far_left(k):
    return 4 if k in (0, 3, 4, 7) else 3


def far_right(k):
    return 7 - far_left(k)


ORDER = (
    (0, 1, 2), (1, 0, 0), (0, 3, 4), (1, 1, 1), (1, 2, 2), (0, 5, 6), (2, 1, 1), (1, 4, 4),
    (0, 7, None), (1, 3, 3), (1, 5, 5), (1, 6, 6), (2, 4, 4), (2, 2, 2), (1, 7, 7), (2, 3, 3),
    (2, 0, 0), (2, 6, 6), (2, 5, 5), (3, 2, 2), (2, 7, 7), (3, 1, 1), (3, 0, 0), (3, 3, 3),
    (3, 6, 6), (3, 4, 4), (3, 5, 5), (3, 7, 7), (4, 3, 2), (4, 0, 1), (4, 4, 5), (4, 7, 6),
)
EVENTS = len(ORDER)


def schedule():
    groups = [(n, n + 1) for n in range(0, EVENTS - 2, BATCH)] + [(EVENTS - 2,), (EVENTS - 1,)]
    steps = [(groups[0], ())]
    for at in range(1, len(groups) - 1):
        steps.append((groups[at], (at - 1,)))
    last = len(groups) - 1
    steps.append((groups[last], (last - 1,)))
    steps.append(((), (last,)))
    return groups, steps


GROUPS, STEPS = schedule()
GROUP_OF = {n: at for at, group in enumerate(GROUPS) for n in group}


def landing_events():
    found = {}
    for n, (j, kl, kr) in enumerate(ORDER):
        found[j, False, kl] = n
        if kr is not None:
            found[j, True, kr] = n
    return found


LANDING = landing_events()


def sends_of(first_z, z, y):
    top_row, low = z == RING - 1, z < 3
    total = 1 + (not (first_z and top_row)) + (not first_z or low) + (first_z or not top_row) + (first_z or low)
    for j, kl, kr in ORDER:
        for right, k in ((False, kl), (True, kr)):
            if k is None:
                continue
            along, across = offset_of(k), j if right else -j
            zz = (z + (along if first_z else across)) % RING
            yy = (y + (across if first_z else along)) % RING
            if j == 0:
                comes = zz < (3 if right else z) if first_z else True
            else:
                comes = zz <= z if first_z else zz < (far_right(k) if right else z)
            if not comes:
                continue
            total += zz * RING + yy < z * RING + y
            if j == 0:
                if k < (5 if right else 7):
                    total += not (first_z and not right and top_row)
                total += zz < z if first_z else not top_row
                total += zz < z if first_z else z < far_right(k)
            elif right:
                total += j < far_right(k)
            elif j < far_left(k):
                total += first_z or not top_row
    return total


TOTALS = sorted({sends_of(f, z, y) for f in (True, False) for z in range(RING) for y in range(RING)})


def kernel(q_raw, k_raw, v_raw, cos_ref, sin_ref, landed, key_ref, q_ref, kv_ref, buf, qbuf, obuf, acc, top, send_sem, own_sem, other_sem, swap_send, swap_recv, out_send, out_recv):
    ctx = lax.axis_index("ctx")
    tp = lax.axis_index("tp")
    core = ctx % 2
    xh = (ctx // 2) % 2
    cell = ctx // 4
    y = cell % RING
    z = cell // RING
    zfirst = core == 0

    def pick(flag, one, two):
        return jnp.where(flag, jnp.int32(one), jnp.int32(two))

    def pick_flag(flag, one, two):
        return pick(flag, one, two) != 0

    def cell_at(dz, dy):
        return ((z + dz + RING) % RING) * RING + (y + dy + RING) % RING

    def dev(at):
        return (at * 4 + xh * 2 + core, tp)

    steps = pick(zfirst, 1, 0)
    a_up = dev(cell_at(steps, 1 - steps))
    a_down = dev(cell_at(-steps, steps - 1))
    b_up = dev(cell_at(1 - steps, steps))
    b_down = dev(cell_at(steps - 1, -steps))
    mate = (cell * 4 + xh * 2 + 1 - core, tp)
    swap = (cell * 4 + (1 - xh) * 2 + core, tp)
    side = (ctx, 1 - tp)
    cross = (cell * 4 + (1 - xh) * 2 + core, 1 - tp)

    barrier = pltpu.get_barrier_semaphore()
    for device in (a_up, a_down, b_up, b_down, mate, swap, side, cross):
        pl.semaphore_signal(barrier, inc=1, device_id=device, device_id_type=MESH)

    cosine = cos_ref[...][:, None, :]
    sine = sin_ref[...][:, None, :]

    def rotated(raw):
        wide = raw[...].astype(jnp.float32)
        return wide * cosine + pltpu.roll(wide, WIDTH // 2, 2) * sine

    keys = rotated(k_raw)
    key_ref[...] = keys.astype(jnp.bfloat16)
    kv_ref[:, :, :WIDTH] = jnp.swapaxes(keys, 0, 1).astype(jnp.bfloat16)
    kv_ref[:, :, WIDTH:] = jnp.swapaxes(v_raw[...].astype(jnp.float32), 0, 1).astype(jnp.bfloat16)
    q_ref[...] = jnp.swapaxes(rotated(q_raw), 0, 1).astype(jnp.bfloat16)

    pl.semaphore_wait(barrier, 8)

    mine = core * CELLS
    theirs = (1 - core) * CELLS
    own = mine + cell
    keep_rows = pl.ds(pl.multiple_of(xh * HALF, HALF), HALF)
    get_rows = pl.ds(pl.multiple_of((1 - xh) * HALF, HALF), HALF)

    def remote(src, dst, s_sem, r_sem, device):
        return pltpu.make_async_remote_copy(
            src_ref=src, dst_ref=dst, send_sem=s_sem, recv_sem=r_sem, device_id=device, device_id_type=MESH
        )

    kv_out = remote(kv_ref.at[1 - xh], buf.at[own, keep_rows], swap_send.at[0], swap_recv.at[0], swap)
    kv_out.start()
    below_top = z < RING - 1
    low = z < 3
    first_targets = (
        (a_up, pick_flag(zfirst, below_top, True)),
        (a_down, pick_flag(zfirst, low, True)),
        (b_up, pick_flag(zfirst, True, below_top)),
        (b_down, pick_flag(zfirst, True, low)),
    )

    halves = (keep_rows, get_rows)
    first_sems = (LANDING[0, False, 1], LANDING[0, True, 2], LANDING[1, False, 0], LANDING[1, True, 0])
    sent = [jnp.int32(1)] + [needed.astype(jnp.int32) for _, needed in first_targets]

    def start_first(src, half):
        part = halves[half]
        for at, (device, needed) in zip(first_sems, first_targets):
            pl.when(needed)(remote(src, buf.at[own, part], send_sem, own_sem.at[half, at], device).start)
        remote(src, buf.at[own, part], send_sem, other_sem.at[len(GROUPS)], mate).start()

    start_first(kv_ref.at[xh], 0)
    other_heads = pl.ds(pl.multiple_of((1 - xh) * GROUP, GROUP), GROUP)
    own_heads = pl.ds(pl.multiple_of(xh * GROUP, GROUP), GROUP)
    q_out = remote(q_ref.at[other_heads], qbuf.at[:, xh], swap_send.at[1], swap_recv.at[1], swap)
    q_out.start()
    buf[own, keep_rows] = kv_ref[xh]
    qbuf[:, xh] = q_ref[own_heads]

    def piece_of(event, right, first_z):
        j, kl, kr = event
        k = kr if right else kl
        if k is None:
            return None
        along = offset_of(k)
        across = j if right else -j
        zz = (z + pick(first_z, along, across) + RING) % RING
        yy = (y + pick(first_z, across, along) + RING) % RING
        at = zz * RING + yy
        if j == 0:
            comes = pick_flag(first_z, zz < (3 if right else z), True)
        else:
            comes = pick_flag(first_z, zz <= z, zz < (far_right(k) if right else z))
        return at, comes, at < cell, zz

    def routes(event, right):
        j, kl, kr = event
        k = kr if right else kl
        zz = piece_of(event, right, zfirst)[3]
        if j == 0:
            ring_end = k >= (5 if right else 7)
            if not ring_end:
                going = pick_flag(zfirst, True if right else below_top, True)
                yield (a_down if right else a_up), going, LANDING[0, right, k + 2]
            yield b_up, pick_flag(zfirst, zz < z, below_top), LANDING[1, False, k]
            yield b_down, pick_flag(zfirst, zz < z, z < far_right(k)), LANDING[1, True, k]
        elif right:
            if j < far_right(k):
                yield b_down, True, LANDING[j + 1, True, k]
        elif j < far_left(k):
            yield b_up, pick_flag(zfirst, True, below_top), LANDING[j + 1, False, k]

    def take(n, half):
        sides = []
        for right in (False, True):
            found = piece_of(ORDER[n], right, zfirst)
            if found is not None:
                sides.append((right,) + found)
        count = sum(comes.astype(jnp.int32) for _, _, comes, _, _ in sides)
        for many in range(1, len(sides) + 1):
            spots = buf.at[pl.ds(0, many), pl.ds(0, HALF)]
            pl.when(count == many)(remote(spots, spots, send_sem, own_sem.at[half, n], b_up).wait_recv)
        for right, at, comes, seen, _ in sides:
            spot = buf.at[mine + at, halves[half]]
            for device, needed, land in routes(ORDER[n], right):
                needed = jnp.logical_and(comes, needed)
                pl.when(needed)(remote(spot, spot, send_sem, own_sem.at[half, land], device).start)
                if half:
                    sent.append(needed.astype(jnp.int32))
            if half:
                needed = jnp.logical_and(comes, seen)
                whole = buf.at[mine + at]
                pl.when(needed)(remote(whole, whole, send_sem, other_sem.at[GROUP_OF[n]], mate).start)
                sent.append(needed.astype(jnp.int32))

    def wait_other(batch, seen):
        count = sum(flag.astype(jnp.int32) for flag in seen)
        for many in range(1, len(seen) + 1):
            spots = buf.at[pl.ds(0, many)]
            pl.when(count == many)(remote(spots, spots, send_sem, other_sem.at[batch], mate).wait_recv)

    for n in GROUPS[0]:
        take(n, 0)

    remote(kv_ref.at[1 - xh], buf.at[own, get_rows], swap_send.at[0], swap_recv.at[0], swap).wait_recv()
    start_first(buf.at[own, get_rows], 1)
    remote(q_ref.at[other_heads], qbuf.at[:, 1 - xh], swap_send.at[1], swap_recv.at[1], swap).wait_recv()

    factor = math.log2(math.e) / math.sqrt(WIDTH)

    def scores_of(keys):
        q = qbuf[...].reshape(ROWS, WIDTH)
        return lax.dot_general(keys, q, (((1,), (1,)), ((), ())), preferred_element_type=jnp.float32)

    def weigh(values, p):
        return lax.dot_general(
            values, p.astype(jnp.bfloat16), (((0,), (0,)), ((), ())), preferred_element_type=jnp.float32
        )

    whole = buf.at[theirs + cell]
    remote(whole, whole, send_sem, other_sem.at[len(GROUPS)], mate).wait_recv()
    key = lax.broadcasted_iota(jnp.int32, (PIECE, ROWS), 0)
    row = lax.broadcasted_iota(jnp.int32, (PIECE, ROWS), 1) % PIECE
    row_at = jnp.where(row < HALF, row, row + HALF) + core * HALF
    key_at = jnp.where(key < HALF, key, key + HALF)
    both = (own, theirs + cell)
    s = scores_of(jnp.concatenate([buf[piece, :, :WIDTH] for piece in both], axis=0))
    s = jnp.concatenate(
        [
            jnp.where(row_at >= key_at + core * HALF, s[:PIECE], -1e30),
            jnp.where(row_at >= key_at + (1 - core) * HALF, s[PIECE:], -1e30),
        ],
        axis=0,
    )
    most = jnp.max(s, axis=0, keepdims=True)
    top[0:1] = most
    p = jnp.exp2((s - most) * factor)
    acc[WIDTH : WIDTH + 1] = jnp.sum(p, axis=0, keepdims=True)
    acc[:WIDTH] = weigh(jnp.concatenate([buf[piece, :, WIDTH:] for piece in both], axis=0), p)

    def attend(pieces):
        some = pieces[0][1]
        for _, seen in pieces[1:]:
            some = jnp.logical_or(some, seen)

        @pl.when(some)
        def _():
            spots = [jnp.where(seen, piece, own) for piece, seen in pieces]
            hide = [jnp.where(seen, 0.0, 1e30) for _, seen in pieces]
            s = scores_of(jnp.concatenate([buf[at, :, :WIDTH] for at in spots], axis=0))
            parts = [s[at * PIECE : (at + 1) * PIECE] for at in range(len(pieces))]
            old = top[0:1]
            new = old
            for part, away in zip(parts, hide):
                new = jnp.maximum(new, jnp.max(part, axis=0, keepdims=True) - away)
            top[0:1] = new
            shrink = jnp.exp2((old - new) * factor)
            p = jnp.concatenate([jnp.exp2((part - (new + away)) * factor) for part, away in zip(parts, hide)], axis=0)
            fresh = weigh(jnp.concatenate([buf[at, :, WIDTH:] for at in spots], axis=0), p)
            acc[WIDTH : WIDTH + 1] = acc[WIDTH : WIDTH + 1] * shrink + jnp.sum(p, axis=0, keepdims=True)
            acc[:WIDTH] = acc[:WIDTH] * shrink + fresh

    for fresh_events, shared in STEPS:
        pieces = []
        for half in (0, 1):
            for n in fresh_events:
                if half or n not in GROUPS[0]:
                    take(n, half)
        for n in fresh_events:
            for right in (False, True):
                found = piece_of(ORDER[n], right, zfirst)
                if found is not None:
                    pieces.append((mine + found[0], found[2]))
        for group in shared:
            theirs_now = []
            for n in GROUPS[group]:
                for right in (False, True):
                    found = piece_of(ORDER[n], right, jnp.logical_not(zfirst))
                    if found is not None:
                        theirs_now.append((theirs + found[0], found[2]))
            wait_other(group, [seen for _, seen in theirs_now])
            pieces += theirs_now
        attend(pieces)

    o = (acc[:WIDTH] / acc[WIDTH : WIDTH + 1]).T.astype(jnp.bfloat16)
    obuf[...] = o.reshape(GROUP, 2, 2, HALF // 2, WIDTH)
    heads = pl.ds(pl.multiple_of(tp * 8 + xh * 4, 4), GROUP)
    places = ((xh, 1 - tp, side), (1 - xh, tp, swap), (1 - xh, 1 - tp, cross))
    for at, (to_xh, to_tp, device) in enumerate(places):
        remote(obuf.at[:, to_xh, to_tp], landed.at[heads], out_send.at[at], out_recv.at[at], device).start()
    landed[heads] = obuf[:, xh, tp]
    kv_out.wait_send()
    q_out.wait_send()
    total = sum(sent)
    for many in TOTALS:
        spots = buf.at[pl.ds(0, many)]
        pl.when(total == many)(remote(spots, spots, send_sem, own_sem.at[0, 0], b_up).wait_send)
    for at, (to_xh, to_tp, device) in enumerate(places):
        from_heads = pl.ds(pl.multiple_of(to_tp * 8 + to_xh * 4, 4), GROUP)
        remote(obuf.at[:, to_xh, to_tp], landed.at[from_heads], out_send.at[at], out_recv.at[at], device).wait()


def finish(by_head, keys, out_ref, key_ref):
    key_ref[...] = keys[...]
    out_ref[...] = jnp.swapaxes(by_head[...].astype(jnp.float32), 0, 1).astype(jnp.bfloat16)


def per_device(queries, incoming_lookup_vectors, incoming_content_vectors):
    tok_rows = queries.shape[0]
    my_index = lax.axis_index("ctx")
    natural_pos = my_index * tok_rows + jnp.arange(tok_rows, dtype=jnp.int32)
    half_width = WIDTH // 2
    inverse_freq = rope_base ** (-(jnp.arange(half_width, dtype=jnp.float32) * 2.0 / WIDTH))
    angles = natural_pos.astype(jnp.float32)[:, None] * inverse_freq[None, :]
    cosine = jnp.cos(angles)
    sine = jnp.sin(angles)
    vmem = pl.BlockSpec(memory_space=pltpu.VMEM)
    by_head, keys = pl.pallas_call(
        kernel,
        out_shape=(
            jax.ShapeDtypeStruct((16, HALF // 2, WIDTH), jnp.bfloat16),
            jax.ShapeDtypeStruct((HALF, 2, WIDTH), jnp.bfloat16),
        ),
        in_specs=[vmem] * 5,
        out_specs=(vmem, vmem),
        scratch_shapes=[
            pltpu.VMEM((8, HALF, WIDTH), jnp.bfloat16),
            pltpu.VMEM((2, HALF, 2 * WIDTH), jnp.bfloat16),
            pltpu.VMEM((2 * CELLS, PIECE, 2 * WIDTH), jnp.bfloat16),
            pltpu.VMEM((GROUP, 2, HALF, WIDTH), jnp.bfloat16),
            pltpu.VMEM((GROUP, 2, 2, HALF // 2, WIDTH), jnp.bfloat16),
            pltpu.VMEM((WIDTH + 8, ROWS), jnp.float32),
            pltpu.VMEM((8, ROWS), jnp.float32),
            pltpu.SemaphoreType.DMA,
            pltpu.SemaphoreType.DMA((2, EVENTS)),
            pltpu.SemaphoreType.DMA((len(GROUPS) + 1,)),
            pltpu.SemaphoreType.DMA((2,)),
            pltpu.SemaphoreType.DMA((2,)),
            pltpu.SemaphoreType.DMA((3,)),
            pltpu.SemaphoreType.DMA((3,)),
        ],
        compiler_params=pltpu.CompilerParams(
            collective_id=0, has_side_effects=True, vmem_limit_bytes=48 * 1024 * 1024
        ),
        name="cell_attention",
    )(
        queries,
        incoming_lookup_vectors,
        incoming_content_vectors,
        jnp.concatenate([cosine, cosine], axis=1),
        jnp.concatenate([-sine, sine], axis=1),
    )
    return pl.pallas_call(
        finish,
        out_shape=(
            jax.ShapeDtypeStruct((HALF // 2, 16, WIDTH), jnp.bfloat16),
            jax.ShapeDtypeStruct((HALF, 2, WIDTH), jnp.bfloat16),
        ),
        in_specs=[vmem] * 2,
        out_specs=(vmem, vmem),
        compiler_params=pltpu.CompilerParams(vmem_limit_bytes=8 * 1024 * 1024),
        name="token_order",
    )(by_head, keys)


def solution(mesh):
    return jax.shard_map(
        per_device,
        mesh=mesh,
        in_specs=(P("ctx", "tp", None), P("ctx", "tp", None), P("ctx", "tp", None)),
        out_specs=(P(("ctx", "tp"), None, None), P("ctx", "tp", None)),
        check_vma=False,
    )
```

```python
import functools
import math

import jax
import jax.numpy as jnp
from jax import lax
from jax.experimental import pallas as pl
from jax.experimental.pallas import tpu as pltpu
from jax.sharding import PartitionSpec as P

MESH = pl.DeviceIdType.MESH
rope_base = 500000.0
RING = 8
CELLS = RING * RING
HALF = 64
PIECE = 2 * HALF
WIDTH = 128
GROUP = 4
ROWS = GROUP * PIECE
BATCH = 2
FEW = 4
WHOLE = 16


def offset_of(k):
    return ((k + 1) // 2) * (1 - 2 * (k % 2))


def far_left(k):
    return 4 if k in (0, 3, 4, 7) else 3


def far_right(k):
    return 7 - far_left(k)


ORDER = (
    (0, 1, 2), (1, 0, 0), (0, 3, 4), (1, 1, 1), (1, 2, 2), (0, 5, 6), (2, 1, 1), (1, 4, 4),
    (0, 7, None), (1, 3, 3), (1, 5, 5), (1, 6, 6), (2, 4, 4), (2, 2, 2), (1, 7, 7), (2, 3, 3),
    (2, 0, 0), (2, 6, 6), (2, 5, 5), (3, 2, 2), (2, 7, 7), (3, 1, 1), (3, 0, 0), (3, 3, 3),
    (3, 6, 6), (3, 4, 4), (3, 5, 5), (3, 7, 7), (4, 3, 2), (4, 0, 1), (4, 4, 5), (4, 7, 6),
)
EVENTS = len(ORDER)


def schedule():
    groups = [(n, n + 1) for n in range(0, EVENTS - 2, BATCH)] + [(EVENTS - 2,), (EVENTS - 1,)]
    steps = [(groups[0], ())]
    for at in range(1, len(groups) - 1):
        steps.append((groups[at], (at - 1,)))
    last = len(groups) - 1
    steps.append((groups[last], (last - 1,)))
    steps.append(((), (last,)))
    return groups, steps


GROUPS, STEPS = schedule()
GROUP_OF = {n: at for at, group in enumerate(GROUPS) for n in group}


def landing_events():
    found = {}
    for n, (j, kl, kr) in enumerate(ORDER):
        found[j, False, kl] = n
        if kr is not None:
            found[j, True, kr] = n
    return found


LANDING = landing_events()


def sends_of(first_z, z, y):
    top_row, low = z == RING - 1, z < 3
    total = 1 + (not (first_z and top_row)) + (not first_z or low) + (first_z or not top_row) + (first_z or low)
    for j, kl, kr in ORDER:
        for right, k in ((False, kl), (True, kr)):
            if k is None:
                continue
            along, across = offset_of(k), j if right else -j
            zz = (z + (along if first_z else across)) % RING
            yy = (y + (across if first_z else along)) % RING
            if j == 0:
                comes = zz < (3 if right else z) if first_z else True
            else:
                comes = zz <= z if first_z else zz < (far_right(k) if right else z)
            if not comes:
                continue
            total += zz * RING + yy < z * RING + y
            if j == 0:
                if k < (5 if right else 7):
                    total += not (first_z and not right and top_row)
                total += zz < z if first_z else not top_row
                total += zz < z if first_z else z < far_right(k)
            elif right:
                total += j < far_right(k)
            elif j < far_left(k):
                total += first_z or not top_row
    return total


TOTALS = sorted({sends_of(f, z, y) for f in (True, False) for z in range(RING) for y in range(RING)})


def kernel(q_raw, k_raw, v_raw, cos_ref, sin_ref, landed, key_ref, q_ref, kv_ref, buf, qbuf, obuf, acc, top, send_sem, own_sem, other_sem, swap_send, swap_recv, out_send, out_recv):
    ctx = lax.axis_index("ctx")
    tp = lax.axis_index("tp")
    core = ctx % 2
    xh = (ctx // 2) % 2
    cell = ctx // 4
    y = cell % RING
    z = cell // RING
    zfirst = core == 0

    def pick(flag, one, two):
        return jnp.where(flag, jnp.int32(one), jnp.int32(two))

    def pick_flag(flag, one, two):
        return pick(flag, one, two) != 0

    def cell_at(dz, dy):
        return ((z + dz + RING) % RING) * RING + (y + dy + RING) % RING

    def dev(at):
        return (at * 4 + xh * 2 + core, tp)

    steps = pick(zfirst, 1, 0)
    a_up = dev(cell_at(steps, 1 - steps))
    a_down = dev(cell_at(-steps, steps - 1))
    b_up = dev(cell_at(1 - steps, steps))
    b_down = dev(cell_at(steps - 1, -steps))
    mate = (cell * 4 + xh * 2 + 1 - core, tp)
    swap = (cell * 4 + (1 - xh) * 2 + core, tp)
    side = (ctx, 1 - tp)
    cross = (cell * 4 + (1 - xh) * 2 + core, 1 - tp)

    barrier = pltpu.get_barrier_semaphore()
    for device in (a_up, a_down, b_up, b_down, mate, swap, side, cross):
        pl.semaphore_signal(barrier, inc=1, device_id=device, device_id_type=MESH)

    cosine = cos_ref[...][:, None, :]
    sine = sin_ref[...][:, None, :]

    def rotated(raw):
        wide = raw[...].astype(jnp.float32)
        return wide * cosine + pltpu.roll(wide, WIDTH // 2, 2) * sine

    keys = rotated(k_raw)
    key_ref[...] = keys.astype(jnp.bfloat16)
    kv_ref[:, :, :WIDTH] = jnp.swapaxes(keys, 0, 1).astype(jnp.bfloat16)
    kv_ref[:, :, WIDTH:] = jnp.swapaxes(v_raw[...].astype(jnp.float32), 0, 1).astype(jnp.bfloat16)
    q_ref[...] = jnp.swapaxes(rotated(q_raw), 0, 1).astype(jnp.bfloat16)

    pl.semaphore_wait(barrier, 8)

    mine = core * CELLS
    theirs = (1 - core) * CELLS
    own = mine + cell
    keep_rows = pl.ds(pl.multiple_of(xh * HALF, HALF), HALF)
    get_rows = pl.ds(pl.multiple_of((1 - xh) * HALF, HALF), HALF)

    def remote(src, dst, s_sem, r_sem, device):
        return pltpu.make_async_remote_copy(
            src_ref=src, dst_ref=dst, send_sem=s_sem, recv_sem=r_sem, device_id=device, device_id_type=MESH
        )

    kv_out = remote(kv_ref.at[1 - xh], buf.at[own, keep_rows], swap_send.at[0], swap_recv.at[0], swap)
    kv_out.start()
    below_top = z < RING - 1
    low = z < 3
    first_targets = (
        (a_up, pick_flag(zfirst, below_top, True)),
        (a_down, pick_flag(zfirst, low, True)),
        (b_up, pick_flag(zfirst, True, below_top)),
        (b_down, pick_flag(zfirst, True, low)),
    )

    halves = (keep_rows, get_rows)
    first_sems = (LANDING[0, False, 1], LANDING[0, True, 2], LANDING[1, False, 0], LANDING[1, True, 0])
    sent = [jnp.int32(1)] + [needed.astype(jnp.int32) for _, needed in first_targets]

    def start_first(src, half):
        part = halves[half]
        for at, (device, needed) in zip(first_sems, first_targets):
            pl.when(needed)(remote(src, buf.at[own, part], send_sem, own_sem.at[half, at], device).start)
        remote(src, buf.at[own, part], send_sem, other_sem.at[len(GROUPS)], mate).start()

    start_first(kv_ref.at[xh], 0)
    other_heads = pl.ds(pl.multiple_of((1 - xh) * GROUP, GROUP), GROUP)
    own_heads = pl.ds(pl.multiple_of(xh * GROUP, GROUP), GROUP)
    q_out = remote(q_ref.at[other_heads], qbuf.at[:, xh], swap_send.at[1], swap_recv.at[1], swap)
    q_out.start()
    buf[own, keep_rows] = kv_ref[xh]
    qbuf[:, xh] = q_ref[own_heads]

    def piece_of(event, right, first_z):
        j, kl, kr = event
        k = kr if right else kl
        if k is None:
            return None
        along = offset_of(k)
        across = j if right else -j
        zz = (z + pick(first_z, along, across) + RING) % RING
        yy = (y + pick(first_z, across, along) + RING) % RING
        at = zz * RING + yy
        if j == 0:
            comes = pick_flag(first_z, zz < (3 if right else z), True)
        else:
            comes = pick_flag(first_z, zz <= z, zz < (far_right(k) if right else z))
        return at, comes, at < cell, zz

    def routes(event, right):
        j, kl, kr = event
        k = kr if right else kl
        zz = piece_of(event, right, zfirst)[3]
        if j == 0:
            ring_end = k >= (5 if right else 7)
            if not ring_end:
                going = pick_flag(zfirst, True if right else below_top, True)
                yield (a_down if right else a_up), going, LANDING[0, right, k + 2]
            yield b_up, pick_flag(zfirst, zz < z, below_top), LANDING[1, False, k]
            yield b_down, pick_flag(zfirst, zz < z, z < far_right(k)), LANDING[1, True, k]
        elif right:
            if j < far_right(k):
                yield b_down, True, LANDING[j + 1, True, k]
        elif j < far_left(k):
            yield b_up, pick_flag(zfirst, True, below_top), LANDING[j + 1, False, k]

    def take(n, half):
        if n >= WHOLE and not half:
            return
        sides = []
        for right in (False, True):
            found = piece_of(ORDER[n], right, zfirst)
            if found is not None:
                sides.append((right,) + found)
        count = sum(comes.astype(jnp.int32) for _, _, comes, _, _ in sides)
        for many in range(1, len(sides) + 1):
            spots = buf.at[pl.ds(0, many), pl.ds(0, PIECE if n >= WHOLE else HALF)]
            pl.when(count == many)(remote(spots, spots, send_sem, own_sem.at[half, n], b_up).wait_recv)
        for right, at, comes, seen, _ in sides:
            for device, needed, land in routes(ORDER[n], right):
                if land >= WHOLE and not half:
                    continue
                spot = buf.at[mine + at] if land >= WHOLE else buf.at[mine + at, halves[half]]
                needed = jnp.logical_and(comes, needed)
                pl.when(needed)(remote(spot, spot, send_sem, own_sem.at[half, land], device).start)
                if half:
                    sent.append(needed.astype(jnp.int32))
            if half:
                needed = jnp.logical_and(comes, seen)
                whole = buf.at[mine + at]
                pl.when(needed)(remote(whole, whole, send_sem, other_sem.at[GROUP_OF[n]], mate).start)
                sent.append(needed.astype(jnp.int32))

    def wait_other(batch, seen):
        count = sum(flag.astype(jnp.int32) for flag in seen)
        for many in range(1, len(seen) + 1):
            spots = buf.at[pl.ds(0, many)]
            pl.when(count == many)(remote(spots, spots, send_sem, other_sem.at[batch], mate).wait_recv)

    for n in GROUPS[0]:
        take(n, 0)

    remote(kv_ref.at[1 - xh], buf.at[own, get_rows], swap_send.at[0], swap_recv.at[0], swap).wait_recv()
    start_first(buf.at[own, get_rows], 1)
    remote(q_ref.at[other_heads], qbuf.at[:, 1 - xh], swap_send.at[1], swap_recv.at[1], swap).wait_recv()

    factor = math.log2(math.e) / math.sqrt(WIDTH)

    def scores_of(keys):
        q = qbuf[...].reshape(ROWS, WIDTH)
        return lax.dot_general(keys, q, (((1,), (1,)), ((), ())), preferred_element_type=jnp.float32)

    def weigh(values, p):
        return lax.dot_general(
            values, p.astype(jnp.bfloat16), (((0,), (0,)), ((), ())), preferred_element_type=jnp.float32
        )

    whole = buf.at[theirs + cell]
    remote(whole, whole, send_sem, other_sem.at[len(GROUPS)], mate).wait_recv()
    key = lax.broadcasted_iota(jnp.int32, (PIECE, ROWS), 0)
    row = lax.broadcasted_iota(jnp.int32, (PIECE, ROWS), 1) % PIECE
    row_at = jnp.where(row < HALF, row, row + HALF) + core * HALF
    key_at = jnp.where(key < HALF, key, key + HALF)
    both = (own, theirs + cell)
    s = scores_of(jnp.concatenate([buf[piece, :, :WIDTH] for piece in both], axis=0))
    s = jnp.concatenate(
        [
            jnp.where(row_at >= key_at + core * HALF, s[:PIECE], -1e30),
            jnp.where(row_at >= key_at + (1 - core) * HALF, s[PIECE:], -1e30),
        ],
        axis=0,
    )
    most = jnp.max(s, axis=0, keepdims=True)
    top[0:1] = most
    p = jnp.exp2((s - most) * factor)
    acc[WIDTH : WIDTH + 1] = jnp.sum(p, axis=0, keepdims=True)
    acc[:WIDTH] = weigh(jnp.concatenate([buf[piece, :, WIDTH:] for piece in both], axis=0), p)

    def attend(pieces):
        count = jnp.int32(0)
        ranks = []
        for _, seen in pieces:
            ranks.append(count)
            count = count + seen.astype(jnp.int32)
        if len(pieces) <= FEW:
            pl.when(count > 0)(functools.partial(attend_to, pieces))
            return
        few = []
        for place in range(FEW):
            at = jnp.int32(0)
            for (piece, seen), rank in zip(pieces, ranks):
                at = at + jnp.where(jnp.logical_and(seen, rank == place), piece, 0)
            few.append((at, place < count))
        pl.when(jnp.logical_and(count > 0, count <= FEW))(functools.partial(attend_to, few))
        pl.when(count > FEW)(functools.partial(attend_to, pieces))

    def attend_to(pieces):
        spots = [jnp.where(seen, piece, own) for piece, seen in pieces]
        hide = [jnp.where(seen, 0.0, 1e30) for _, seen in pieces]
        s = scores_of(jnp.concatenate([buf[at, :, :WIDTH] for at in spots], axis=0))
        parts = [s[at * PIECE : (at + 1) * PIECE] for at in range(len(pieces))]
        old = top[0:1]
        new = old
        for part, away in zip(parts, hide):
            new = jnp.maximum(new, jnp.max(part, axis=0, keepdims=True) - away)
        top[0:1] = new
        shrink = jnp.exp2((old - new) * factor)
        p = jnp.concatenate([jnp.exp2((part - (new + away)) * factor) for part, away in zip(parts, hide)], axis=0)
        fresh = weigh(jnp.concatenate([buf[at, :, WIDTH:] for at in spots], axis=0), p)
        acc[WIDTH : WIDTH + 1] = acc[WIDTH : WIDTH + 1] * shrink + jnp.sum(p, axis=0, keepdims=True)
        acc[:WIDTH] = acc[:WIDTH] * shrink + fresh

    for fresh_events, shared in STEPS:
        pieces = []
        for half in (0, 1):
            for n in fresh_events:
                if half or n not in GROUPS[0]:
                    take(n, half)
        for n in fresh_events:
            for right in (False, True):
                found = piece_of(ORDER[n], right, zfirst)
                if found is not None:
                    pieces.append((mine + found[0], found[2]))
        for group in shared:
            theirs_now = []
            for n in GROUPS[group]:
                for right in (False, True):
                    found = piece_of(ORDER[n], right, jnp.logical_not(zfirst))
                    if found is not None:
                        theirs_now.append((theirs + found[0], found[2]))
            wait_other(group, [seen for _, seen in theirs_now])
            pieces += theirs_now
        attend(pieces)

    o = (acc[:WIDTH] / acc[WIDTH : WIDTH + 1]).T.astype(jnp.bfloat16)
    obuf[...] = o.reshape(GROUP, 2, 2, HALF // 2, WIDTH)
    heads = pl.ds(pl.multiple_of(tp * 8 + xh * 4, 4), GROUP)
    places = ((xh, 1 - tp, side), (1 - xh, tp, swap), (1 - xh, 1 - tp, cross))
    for at, (to_xh, to_tp, device) in enumerate(places):
        remote(obuf.at[:, to_xh, to_tp], landed.at[heads], out_send.at[at], out_recv.at[at], device).start()
    landed[heads] = obuf[:, xh, tp]
    kv_out.wait_send()
    q_out.wait_send()
    total = sum(sent)
    for many in TOTALS:
        spots = buf.at[pl.ds(0, many)]
        pl.when(total == many)(remote(spots, spots, send_sem, own_sem.at[0, 0], b_up).wait_send)
    for at, (to_xh, to_tp, device) in enumerate(places):
        from_heads = pl.ds(pl.multiple_of(to_tp * 8 + to_xh * 4, 4), GROUP)
        remote(obuf.at[:, to_xh, to_tp], landed.at[from_heads], out_send.at[at], out_recv.at[at], device).wait()


def finish(by_head, keys, out_ref, key_ref):
    key_ref[...] = keys[...]
    out_ref[...] = jnp.swapaxes(by_head[...].astype(jnp.float32), 0, 1).astype(jnp.bfloat16)


def per_device(queries, incoming_lookup_vectors, incoming_content_vectors):
    tok_rows = queries.shape[0]
    my_index = lax.axis_index("ctx")
    natural_pos = my_index * tok_rows + jnp.arange(tok_rows, dtype=jnp.int32)
    half_width = WIDTH // 2
    inverse_freq = rope_base ** (-(jnp.arange(half_width, dtype=jnp.float32) * 2.0 / WIDTH))
    angles = natural_pos.astype(jnp.float32)[:, None] * inverse_freq[None, :]
    cosine = jnp.cos(angles)
    sine = jnp.sin(angles)
    vmem = pl.BlockSpec(memory_space=pltpu.VMEM)
    by_head, keys = pl.pallas_call(
        kernel,
        out_shape=(
            jax.ShapeDtypeStruct((16, HALF // 2, WIDTH), jnp.bfloat16),
            jax.ShapeDtypeStruct((HALF, 2, WIDTH), jnp.bfloat16),
        ),
        in_specs=[vmem] * 5,
        out_specs=(vmem, vmem),
        scratch_shapes=[
            pltpu.VMEM((8, HALF, WIDTH), jnp.bfloat16),
            pltpu.VMEM((2, HALF, 2 * WIDTH), jnp.bfloat16),
            pltpu.VMEM((2 * CELLS, PIECE, 2 * WIDTH), jnp.bfloat16),
            pltpu.VMEM((GROUP, 2, HALF, WIDTH), jnp.bfloat16),
            pltpu.VMEM((GROUP, 2, 2, HALF // 2, WIDTH), jnp.bfloat16),
            pltpu.VMEM((WIDTH + 8, ROWS), jnp.float32),
            pltpu.VMEM((8, ROWS), jnp.float32),
            pltpu.SemaphoreType.DMA,
            pltpu.SemaphoreType.DMA((2, EVENTS)),
            pltpu.SemaphoreType.DMA((len(GROUPS) + 1,)),
            pltpu.SemaphoreType.DMA((2,)),
            pltpu.SemaphoreType.DMA((2,)),
            pltpu.SemaphoreType.DMA((3,)),
            pltpu.SemaphoreType.DMA((3,)),
        ],
        compiler_params=pltpu.CompilerParams(
            collective_id=0, has_side_effects=True, vmem_limit_bytes=48 * 1024 * 1024
        ),
        name="cell_attention",
    )(
        queries,
        incoming_lookup_vectors,
        incoming_content_vectors,
        jnp.concatenate([cosine, cosine], axis=1),
        jnp.concatenate([-sine, sine], axis=1),
    )
    return pl.pallas_call(
        finish,
        out_shape=(
            jax.ShapeDtypeStruct((HALF // 2, 16, WIDTH), jnp.bfloat16),
            jax.ShapeDtypeStruct((HALF, 2, WIDTH), jnp.bfloat16),
        ),
        in_specs=[vmem] * 2,
        out_specs=(vmem, vmem),
        compiler_params=pltpu.CompilerParams(vmem_limit_bytes=8 * 1024 * 1024),
        name="token_order",
    )(by_head, keys)


def solution(mesh):
    return jax.shard_map(
        per_device,
        mesh=mesh,
        in_specs=(P("ctx", "tp", None), P("ctx", "tp", None), P("ctx", "tp", None)),
        out_specs=(P(("ctx", "tp"), None, None), P("ctx", "tp", None)),
        check_vma=False,
    )
```
